32 devices in a mesh: groups: 2 (over x), tensor: 8 (over z, y), batch: 2 (over core).
Axes of the slice: x: 2, y: 2, z: 4, core: 2. Of those that a mesh axis runs over, the one named last changes fastest.
Arguments:
- hidden: bfloat16 [256, 2, 8192], P(('groups', 'tensor', 'batch')), parts along dimension 0, may hold values from -6 to 6
- wq: bfloat16 [8192, 8192], P(None, 'tensor'), may hold values from -0.0625 to 0.0625
- wkv: bfloat16 [8192, 2048], P(None, 'tensor'), may hold values from -0.0625 to 0.0625
- cache_pool: bfloat16 [512, 128, 2048], P(('groups', 'tensor', 'batch')), parts along dimension 0, may hold values from -240 to 240
- page_table: int32 [256, 2], P(('groups', 'tensor', 'batch')), parts along dimension 0, may hold values from 0 to 15, as said below
- ctx_len: int32 [256], P(('groups', 'tensor', 'batch')), parts along dimension 0, may hold values from 1 to 256
- prompt_slot: int32 [32], P(('groups', 'tensor', 'batch')), parts along dimension 0, may hold values from 0 to 7
- prompt_kv: bfloat16 [32, 128, 2048], P(('groups', 'batch'), None, 'tensor'), parts along dimension 0, may hold values from -6 to 6
Outputs:
- attended: bfloat16 [256, 2, 8192], P(('groups', 'tensor', 'batch')), parts along dimension 0
The draws below stay inside these ranges and needn't reach their ends.
There are 2 independent parts, one for each index of `groups`. The reference program is written for one: setup_inputs(seed, part) draws one part's arguments, and reference() takes and returns one part's arrays. A program takes and returns all parts, laid end to end along the dimension named above; an argument that names none is the same for every part. Nothing has to cross between parts.
Inputs may be any that keep to these rules, and one draw needn't show every extreme that they name: `page_table`: within each block of 8 sequences the entries name each of that block's 16 local pages exactly once; entry p holds the sequence's tokens p * 128 to (p + 1) * 128 - 1.
All inputs are finite; a program needn't handle non-finite values.
Results may differ from the reference program's by a relative error of at most 0.012.
Values may be sent and summed in bfloat16 or wider, within the bound.
A program may use at most 128 MiB of HBM per device.

```python
import jax
import jax.numpy as jnp
from jax import lax

D = 8192
QUERY_HEADS = 64
KEY_VALUE_HEADS = 8
HEAD_SIZE = 128
PAGE = 128
SEQ_PAGES = 2
PLEN = 128
SEQ_DEV = 8
KEY_VALUE_WIDTH = 2048
POOL_DEV = 16
SEQS = 128
PROMPTS = 16
POOLS = 256
N_TENSOR = 8
N_BATCH = 2


def draw_cache_pool(key, part):
    base = jnp.clip(jax.random.normal(key, (POOLS, PAGE, KEY_VALUE_WIDTH), jnp.float32), -4.0, 4.0)
    return base.astype(jnp.bfloat16)


def draw_page_table(key, part):
    blocks = SEQS // SEQ_DEV
    subkeys = jax.random.split(jax.random.fold_in(key, 3), blocks)
    orders = jax.vmap(lambda single: jax.random.permutation(single, POOL_DEV))(subkeys)
    return orders.reshape(SEQS, SEQ_PAGES).astype(jnp.int32)


def touch_ends(values, key, low, high):
    longest = values.shape.index(max(values.shape))
    spots = []
    for shift in (0, 1):
        where = [jax.random.randint(jax.random.fold_in(key, axis), (), 0, length) for axis, length in enumerate(values.shape)]
        where[longest] = (where[longest] + shift) % values.shape[longest]
        spots.append(tuple(where))
    return values.at[spots[0]].set(low).at[spots[1]].set(high)


def block_scale(stream_key, shape, pieces, smallest, top_value):
    def one(dim, shards_of):
        draws = jax.random.uniform(jax.random.fold_in(jax.random.fold_in(stream_key, 6), dim), (shards_of,), jnp.float32, smallest / len(pieces), top_value / len(pieces))
        return jnp.repeat(jnp.exp(draws), shape[dim] // shards_of).reshape((-1,) + (1,) * (len(shape) - dim - 1))

    gain = one(*pieces[0])
    for cut in pieces[1:]:
        gain = gain * one(*cut)
    return gain


def gaussian(key, shape, width, reach, cuts=(), kind=jnp.bfloat16):
    entries = jax.random.normal(key, shape, jnp.float32) * width
    if len(cuts) > 0:
        entries = block_scale(key, shape, cuts, -0.22, 0.18) * entries
    return jnp.clip(entries, min=-reach, max=reach).astype(kind)


def setup_inputs(seed: int = 0, part: int = 0) -> dict:
    key_list = jax.random.split(jax.random.key(seed), 9)
    part_splits = jax.random.split(jax.random.fold_in(key_list[8], part), 9)
    return {
        "hidden": gaussian(part_splits[0], (SEQS, 2, D), 1.0, 6.0, ((0, 16),)),
        "wq": gaussian(key_list[1], (D, QUERY_HEADS * HEAD_SIZE), D ** -0.5, 0.0625, ((1, 8),)),
        "wkv": gaussian(key_list[2], (D, KEY_VALUE_WIDTH), D ** -0.5, 0.0625, ((1, 8),)),
        "cache_pool": draw_cache_pool(jax.random.fold_in(jax.random.fold_in(key_list[8], part), 71), part),
        "page_table": draw_page_table(jax.random.fold_in(jax.random.fold_in(key_list[8], part), 71), part),
        "ctx_len": touch_ends(jax.random.randint(part_splits[5], (SEQS,), 1, SEQ_PAGES * PAGE + 1), jax.random.fold_in(part_splits[5], 1), 1, SEQ_PAGES * PAGE).astype(jnp.int32),
        "prompt_slot": touch_ends(jax.random.randint(part_splits[6], (PROMPTS,), 0, SEQ_DEV), jax.random.fold_in(part_splits[6], 1), 0, SEQ_DEV - 1).astype(jnp.int32),
        "prompt_kv": gaussian(part_splits[7], (PROMPTS, PLEN, KEY_VALUE_WIDTH), 1.0, 6.0, ((0, 2), (2, 8))),
    }


def attend_block(query_rows, kv_new, prompt, pool, table, lens, slot):
    token_count = query_rows.shape[0]
    span = SEQ_PAGES * PAGE
    context = pool[table].reshape(token_count, span, KEY_VALUE_WIDTH)
    prompt_rows = jnp.broadcast_to(prompt[None], (token_count, PLEN, KEY_VALUE_WIDTH))
    combined_keys = jnp.concatenate([context, prompt_rows, kv_new], axis=1)
    valid_length = combined_keys.shape[1]
    where_key = jnp.arange(valid_length, dtype=jnp.int32)
    seq_local = jnp.arange(token_count, dtype=jnp.int32)
    step_ids = jnp.arange(2, dtype=jnp.int32)
    in_context = (where_key < span)[None, None, :]
    in_prompt = ((where_key >= span) & (where_key < span + PLEN))[None, None, :]
    context_ok = (where_key[None, :] < lens[:, None])[:, None, :]
    prompt_ok = (seq_local == slot)[:, None, None]
    new_ok = ((where_key - span - PLEN)[None, None, :] <= step_ids[None, :, None])
    live = jnp.where(in_context, context_ok, jnp.where(in_prompt, prompt_ok, new_ok))
    key_rows = combined_keys[:, :, :KEY_VALUE_HEADS * HEAD_SIZE].reshape(token_count, valid_length, KEY_VALUE_HEADS, HEAD_SIZE).astype(jnp.float32)
    value_rows = combined_keys[:, :, KEY_VALUE_HEADS * HEAD_SIZE:].reshape(token_count, valid_length, KEY_VALUE_HEADS, HEAD_SIZE).astype(jnp.float32)
    head_group = query_rows.reshape(token_count, 2, KEY_VALUE_HEADS, QUERY_HEADS // KEY_VALUE_HEADS, HEAD_SIZE).astype(jnp.float32)
    scores = jnp.einsum('sikgd,slkd->sikgl', head_group, key_rows) * (HEAD_SIZE ** -0.5)
    scores = jnp.where(live[:, :, None, None, :], scores, -1e30)
    top = jnp.max(scores, axis=-1, keepdims=True)
    expo = jnp.exp(scores - top)
    weights = (expo / jnp.sum(expo, axis=-1, keepdims=True)).astype(jnp.bfloat16)
    result = jnp.einsum('sikgl,slkd->sikgd', weights.astype(jnp.float32), value_rows)
    return result.astype(jnp.bfloat16).reshape(token_count, 2, QUERY_HEADS * HEAD_SIZE)


def reference(hidden, wq, wkv, cache_pool, page_table, ctx_len, prompt_slot, prompt_kv):
    blocks = N_TENSOR * N_BATCH
    flat = hidden.reshape(SEQS * 2, D)
    query_rows = jnp.dot(flat, wq, preferred_element_type=jnp.float32).astype(jnp.bfloat16)
    kv_new = jnp.dot(flat, wkv, preferred_element_type=jnp.float32).astype(jnp.bfloat16)
    query_rows = query_rows.reshape(blocks, SEQ_DEV, 2, QUERY_HEADS * HEAD_SIZE)
    kv_new = kv_new.reshape(blocks, SEQ_DEV, 2, KEY_VALUE_WIDTH)
    block_ids = jnp.arange(blocks, dtype=jnp.int32)
    owner = (block_ids % N_BATCH) * N_TENSOR + block_ids // N_BATCH
    prompts = prompt_kv[owner.astype(jnp.int32)]
    pools = cache_pool.reshape(blocks, POOL_DEV, PAGE, KEY_VALUE_WIDTH)
    tables = page_table.reshape(blocks, SEQ_DEV, SEQ_PAGES)
    lengths = ctx_len.reshape(blocks, SEQ_DEV)

    def one_block(items):
        return attend_block(*items)

    result = lax.map(one_block, (query_rows, kv_new, prompts, pools, tables, lengths, prompt_slot))
    return result.reshape(SEQS, 2, QUERY_HEADS * HEAD_SIZE)
```

```python
import functools

import jax
import jax.numpy as jnp
from jax import lax
from jax.experimental import pallas as pl
from jax.experimental.pallas import tpu as pltpu
from jax.sharding import PartitionSpec as P

QUERY_HEADS = 64
KEY_VALUE_HEADS = 8
HEAD_SIZE = 128
GROUP = QUERY_HEADS // KEY_VALUE_HEADS
MESH = pl.DeviceIdType.MESH
NEG = -1e30
UNROLL = 2


def dot_t(a, b):
    return lax.dot_general(a, b, (((1,), (1,)), ((), ())), preferred_element_type=jnp.float32)


def attend_kernel(
    seqs, pages, table, lens, slot, *refs
):
    page_refs = refs[:pages]
    q_ref, kv_ref, prompt_ref, out_ref, qp, op = refs[pages:]
    s = pl.program_id(0)
    rows = seqs * 2
    block = 2 * GROUP
    total = rows * GROUP
    kv_half = KEY_VALUE_HEADS * HEAD_SIZE

    def perm(transposed):
        r = lax.broadcasted_iota(jnp.int32, (total, total), 1 if transposed else 0)
        c = lax.broadcasted_iota(jnp.int32, (total, total), 0 if transposed else 1)
        seq, rest = r // block, r % block
        source = (rest % GROUP) * rows + seq * 2 + rest // GROUP
        return jnp.where(c == source, 1.0, 0.0).astype(jnp.bfloat16)

    @pl.when(s == 0)
    def _():
        p = perm(False)
        for h in range(KEY_VALUE_HEADS):
            tiles = [
                q_ref[:, (h * GROUP + g) * HEAD_SIZE : (h * GROUP + g + 1) * HEAD_SIZE]
                for g in range(GROUP)
            ]
            stacked = jnp.concatenate(tiles, axis=0)
            qp[h] = jnp.dot(p, stacked, preferred_element_type=jnp.float32).astype(jnp.bfloat16)

    page_rows = page_refs[0].shape[1]
    length = lens[s]
    lane = lax.broadcasted_iota(jnp.int32, (block, page_rows), 1)
    new_col = lax.broadcasted_iota(jnp.int32, (block, rows), 1)
    new_row = lax.broadcasted_iota(jnp.int32, (block, rows), 0)
    new_live = (new_col // 2 == s) & (new_col % 2 <= new_row // GROUP)
    here = pl.ds(pl.multiple_of(s * block, block), block)
    scale = HEAD_SIZE ** (-0.5)

    def heads(with_prompt):
        for h in range(KEY_VALUE_HEADS):
            kc = slice(h * HEAD_SIZE, (h + 1) * HEAD_SIZE)
            vc = slice(kv_half + h * HEAD_SIZE, kv_half + (h + 1) * HEAD_SIZE)
            qh = qp[h, here, :]
            parts = []
            for p in range(pages):
                sc = dot_t(qh, page_refs[p][0, :, kc]) * scale
                parts.append((jnp.where(lane + p * page_rows < length, sc, NEG), page_refs[p][0, :, vc]))
            sc = dot_t(qh, kv_ref[:, kc]) * scale
            parts.append((jnp.where(new_live, sc, NEG), kv_ref[:, vc]))
            if with_prompt:
                parts.append((dot_t(qh, prompt_ref[:, kc]) * scale, prompt_ref[:, vc]))
            top = functools.reduce(
                jnp.maximum, [jnp.max(sc, axis=-1, keepdims=True) for sc, _ in parts]
            )
            expo = [jnp.exp(sc - top) for sc, _ in parts]
            norm = functools.reduce(
                jnp.add, [jnp.sum(e, axis=-1, keepdims=True) for e in expo]
            )
            acc = functools.reduce(
                jnp.add,
                [
                    jnp.dot(e.astype(jnp.bfloat16), v, preferred_element_type=jnp.float32)
                    for e, (_, v) in zip(expo, parts)
                ],
            )
            op[h, here, :] = (acc / norm).astype(jnp.bfloat16)

    mine = s == slot[0]

    @pl.when(mine)
    def _():
        heads(True)

    @pl.when(jnp.logical_not(mine))
    def _():
        heads(False)

    @pl.when(s == seqs - 1)
    def _():
        p = perm(True)
        for h in range(KEY_VALUE_HEADS):
            back = jnp.dot(p, op[h], preferred_element_type=jnp.float32).astype(jnp.bfloat16)
            for g in range(GROUP):
                out_ref[:, (h * GROUP + g) * HEAD_SIZE : (h * GROUP + g + 1) * HEAD_SIZE] = back[
                    g * rows : (g + 1) * rows, :
                ]


def attend(query, keyval, prompt, pool, table, lens, slot):
    seqs, pages = table.shape
    page_rows, kv_cols = pool.shape[1:]
    rows = query.shape[0]

    def page_spec(p):
        return pl.BlockSpec((1, page_rows, kv_cols), lambda s, t, l, sl: (t[s * pages + p], 0, 0))

    def whole(x):
        return pl.BlockSpec(x.shape, lambda s, t, l, sl: (0,) * x.ndim)

    total = rows * GROUP
    return pl.pallas_call(
        functools.partial(attend_kernel, seqs, pages),
        grid_spec=pltpu.PrefetchScalarGridSpec(
            num_scalar_prefetch=3,
            grid=(seqs,),
            in_specs=[page_spec(p) for p in range(pages)] + [whole(query), whole(keyval), whole(prompt)],
            out_specs=pl.BlockSpec(query.shape, lambda s, t, l, sl: (0, 0)),
            scratch_shapes=[
                pltpu.VMEM((KEY_VALUE_HEADS, total, HEAD_SIZE), jnp.bfloat16),
                pltpu.VMEM((KEY_VALUE_HEADS, total, HEAD_SIZE), jnp.bfloat16),
            ],
        ),
        out_shape=jax.ShapeDtypeStruct(query.shape, jnp.bfloat16),
        compiler_params=pltpu.CompilerParams(dimension_semantics=("arbitrary",)),
        name="attend",
    )(table.reshape(-1), lens, slot, *([pool] * pages), query, keyval, prompt)


def attend_resident(table, lens, slot, pool_v, q_out, kv_out, prompt_out, qbd, op, out, after):
    seqs = lens.shape[0]
    pages = table.shape[0]
    rows = seqs * 2
    block = 2 * GROUP
    total = rows * GROUP
    kv_half = KEY_VALUE_HEADS * HEAD_SIZE
    page_rows = pool_v.shape[1]
    lanes = KEY_VALUE_HEADS * block
    scale = HEAD_SIZE ** (-0.5)

    def perm(transposed):
        r = lax.broadcasted_iota(jnp.int32, (total, total), 1 if transposed else 0)
        c = lax.broadcasted_iota(jnp.int32, (total, total), 0 if transposed else 1)
        seq, rest = r // block, r % block
        source = (rest % GROUP) * rows + seq * 2 + rest // GROUP
        return jnp.where(c == source, 1.0, 0.0).astype(jnp.bfloat16)

    p = perm(False)
    for h in range(KEY_VALUE_HEADS):
        tiles = [
            q_out[:, (h * GROUP + g) * HEAD_SIZE : (h * GROUP + g + 1) * HEAD_SIZE]
            for g in range(GROUP)
        ]
        ordered = jnp.dot(
            p, jnp.concatenate(tiles, axis=0), preferred_element_type=jnp.float32
        ).astype(jnp.bfloat16)
        for s in range(seqs):
            qbd[s, h * block : (h + 1) * block, h * HEAD_SIZE : (h + 1) * HEAD_SIZE] = ordered[
                s * block : (s + 1) * block, :
            ]

    key = lax.broadcasted_iota(jnp.int32, (page_rows, lanes), 0)
    new_key = lax.broadcasted_iota(jnp.int32, (rows, lanes), 0)
    new_pos = lax.broadcasted_iota(jnp.int32, (rows, lanes), 1) // GROUP % 2

    def one(s, with_prompt):
        q = qbd[s]
        where_pages = [table[p, s] for p in range(pages)]
        parts = []
        for p in range(pages):
            sc = dot_t(pool_v[where_pages[p], :, :kv_half], q) * scale
            parts.append(jnp.where(key + p * page_rows < lens[s], sc, NEG))
        if with_prompt:
            parts.append(dot_t(prompt_out[:, :kv_half], q) * scale)
        sc = dot_t(kv_out[:, :kv_half], q) * scale
        parts.append(jnp.where((new_key // 2 == s) & (new_key % 2 <= new_pos), sc, NEG))
        top = functools.reduce(jnp.maximum, [jnp.max(x, axis=0, keepdims=True) for x in parts])
        expo = [jnp.exp(x - top) for x in parts]
        norm = functools.reduce(jnp.add, [jnp.sum(e, axis=0, keepdims=True) for e in expo])
        weights = [jnp.transpose(e / norm).astype(jnp.bfloat16) for e in expo]
        wide = jnp.concatenate(weights[:pages], axis=1)
        outs = []
        for h in range(KEY_VALUE_HEADS):
            vc = slice(kv_half + h * HEAD_SIZE, kv_half + (h + 1) * HEAD_SIZE)
            mine = slice(h * block, (h + 1) * block)
            v = jnp.concatenate([pool_v[w, :, vc] for w in where_pages], axis=0)
            acc = jnp.dot(wide[mine], v, preferred_element_type=jnp.float32)
            acc += jnp.dot(weights[-1][mine], kv_out[:, vc], preferred_element_type=jnp.float32)
            if with_prompt:
                acc += jnp.dot(weights[pages][mine], prompt_out[:, vc], preferred_element_type=jnp.float32)
            outs.append(acc.astype(jnp.bfloat16))
        return outs

    def several(k, carry):
        for u in range(UNROLL):
            s = k * UNROLL + u
            for h, o in enumerate(one(s, False)):
                op[h, pl.ds(pl.multiple_of(s * block, block), block), :] = o
        return carry

    lax.fori_loop(0, seqs // UNROLL, several, 0)
    after()
    chosen = slot[0]
    continued = one(chosen, True)
    row_seq = lax.broadcasted_iota(jnp.int32, (total, HEAD_SIZE), 0) // block
    p = perm(True)
    for h in range(KEY_VALUE_HEADS):
        spread = jnp.concatenate([continued[h]] * seqs, axis=0)
        mixed = jnp.where(row_seq == chosen, spread, op[h])
        back = jnp.dot(p, mixed, preferred_element_type=jnp.float32).astype(jnp.bfloat16)
        for g in range(GROUP):
            out[:, (h * GROUP + g) * HEAD_SIZE : (h * GROUP + g + 1) * HEAD_SIZE] = back[
                g * rows : (g + 1) * rows, :
            ]


def relay_kernel(
    n, chunks, table_h, lens_h, slot_h, hidden, wq, wkv, prompt, pool, attended,
    table, lens, slot, hid_v,
    q_out, kv_out, prompt_out, prompt_v, pool_v, qbd, op,
    gath, wq_v, wkv_v, acc_q, acc_kv, stage_q, stage_kv,
    right_send, right_recv, left_send, left_recv,
    q_send, q_recv, kv_send, kv_recv, p_send, p_recv, w_sem, local_sem,
):
    me = lax.axis_index("tensor")
    rows, depth = attended.shape[0], hidden.shape[2]
    width = depth // chunks
    q_cols, kv_cols = wq.shape[1], wkv.shape[1]
    half = n // 2
    pos = jnp.where(me % 2 == 0, me // 2, n - 1 - me // 2)

    def at(position):
        p = lax.rem(position + 2 * n, n)
        return jnp.where(p < half, 2 * p, 2 * (n - 1 - p) + 1)

    def slot_of(direction, hop):
        return 0 if hop == 0 else n - 1 if hop == half else 2 * hop - 1 + direction

    def rows_of(k, count=1):
        return pl.ds(k * rows, count * rows)

    barrier = pltpu.get_barrier_semaphore()
    for sign in (-1, 1):
        pl.semaphore_signal(
            barrier, inc=1, device_id={"tensor": at(pos + sign)}, device_id_type=MESH
        )
    own = pltpu.make_async_copy(hidden, hid_v, local_sem.at[0])
    own.start()
    scalars = []
    for k, (src, dst) in enumerate(((table_h, table), (lens_h, lens), (slot_h, slot))):
        copy = pltpu.make_async_copy(src, dst, local_sem.at[1 + k])
        copy.start()
        scalars.append(copy)
    weights = []
    for c in range(chunks):
        k = pl.ds(c * width, width)
        pair = (
            pltpu.make_async_copy(wq.at[k, :], wq_v.at[k, :], w_sem.at[0, c]),
            pltpu.make_async_copy(wkv.at[k, :], wkv_v.at[k, :], w_sem.at[1, c]),
        )
        for copy in pair:
            copy.start()
        weights.append(pair)
    load_prompt = pltpu.make_async_copy(prompt, prompt_v, local_sem.at[4])
    load_prompt.start()
    load_pool = pltpu.make_async_copy(pool, pool_v, local_sem.at[5])
    load_pool.start()

    def goes(direction, hop, c):
        return hop < half or (hop == half and c % 2 == direction)

    def ring_copy(direction, hop, c):
        sign = 1 if direction == 0 else -1
        cols = pl.ds(c * width, width)
        send, recv = (right_send, right_recv) if direction == 0 else (left_send, left_recv)
        return pltpu.make_async_remote_copy(
            src_ref=gath.at[rows_of(slot_of(direction, hop - 1)), cols],
            dst_ref=gath.at[rows_of(slot_of(direction, hop)), cols],
            send_sem=send.at[hop - 1, c],
            recv_sem=recv.at[hop - 1, c],
            device_id={"tensor": at(pos + sign)},
            device_id_type=MESH,
        )

    started = {}

    def launch(hop, c):
        for direction in (0, 1):
            if goes(direction, hop, c):
                copy = ring_copy(direction, hop, c)
                copy.start()
                started[direction, hop, c] = copy

    def arrive(hop, c):
        for direction in (0, 1):
            if goes(direction, hop, c):
                started[direction, hop, c].wait_recv()

    def multiply(first, count, c):
        if first == 0:
            for copy in weights[c]:
                copy.wait()
        taken = slice(first * rows, (first + count) * rows)
        x = gath[taken, c * width : (c + 1) * width]
        for w, acc in ((wq_v, acc_q), (wkv_v, acc_kv)):
            part = jnp.dot(x, w[c * width : (c + 1) * width, :], preferred_element_type=jnp.float32)
            if c == 0:
                acc[taken, :] = part
            else:
                acc[taken, :] += part

    results = []

    def hand_out(first, count):
        taken = slice(first * rows, (first + count) * rows)
        stage_q[taken, :] = acc_q[taken, :].astype(jnp.bfloat16)
        stage_kv[taken, :] = acc_kv[taken, :].astype(jnp.bfloat16)
        for k in range(max(first, 1), first + count):
            hops = (k + 1) // 2
            t = at(pos - hops if k % 2 == 1 else pos + hops)
            for stage, out, cols, send, recv in (
                (stage_q, q_out, q_cols, q_send, q_recv),
                (stage_kv, kv_out, kv_cols, kv_send, kv_recv),
            ):
                copy = pltpu.make_async_remote_copy(
                    src_ref=stage.at[rows_of(k), :],
                    dst_ref=out.at[:, pl.ds(pl.multiple_of(me * cols, cols), cols)],
                    send_sem=send.at[k],
                    recv_sem=recv.at[k],
                    device_id={"tensor": t},
                    device_id_type=MESH,
                )
                copy.start()
                results.append(copy)

    own.wait()
    for c in range(chunks):
        cols = slice(c * width, (c + 1) * width)
        gath[rows_of(0), cols] = hid_v[:, :, cols].reshape(rows, width)
    pl.semaphore_wait(barrier, 2)
    for c in range(chunks):
        launch(1, c)
    qbd[...] = jnp.zeros_like(qbd)
    load_prompt.wait()
    for hop in range(1, half - 1):
        for c in range(chunks):
            arrive(hop, c)
            launch(hop + 1, c)
    early = 2 * (half - 2) + 1
    for c in range(chunks):
        multiply(0, early, c)
        arrive(half - 1, c)
        launch(half, c)
    hand_out(0, early)
    for c in range(chunks):
        arrive(half, c)
        multiply(early, n - early, c)
    hand_out(early, n - early)
    prompts = []
    for d in range(1, n):
        t = lax.rem(me + d, n)
        copy = pltpu.make_async_remote_copy(
            src_ref=prompt_v.at[t],
            dst_ref=prompt_out.at[:, pl.ds(pl.multiple_of(me * kv_cols, kv_cols), kv_cols)],
            send_sem=p_send.at[d],
            recv_sem=p_recv.at[d],
            device_id={"tensor": t},
            device_id_type=MESH,
        )
        prompts.append(copy)
    for copy in prompts:
        copy.start()
    for source, out, cols in (
        (stage_q[0:rows, :], q_out, q_cols),
        (stage_kv[0:rows, :], kv_out, kv_cols),
        (prompt_v[me], prompt_out, kv_cols),
    ):
        out[:, pl.ds(pl.multiple_of(me * cols, cols), cols)] = source
    for copy in results:
        copy.wait()
    for copy in scalars:
        copy.wait()
    load_pool.wait()

    def after():
        for copy in prompts:
            copy.wait()

    attend_resident(
        table, lens, slot, pool_v, q_out, kv_out, prompt_out, qbd, op, attended, after
    )
    for copy in started.values():
        copy.wait_send()


def relay(hidden, wq, wkv, prompt, pool, table, lens, slot, n):
    seqs, per, depth = hidden.shape
    rows = seqs * per
    q_cols, kv_cols = wq.shape[1], wkv.shape[1]
    chunks = 8
    half = n // 2
    vmem = pl.BlockSpec(memory_space=pltpu.VMEM)
    hbm = pl.BlockSpec(memory_space=pltpu.HBM)
    dma = pltpu.SemaphoreType.DMA
    plen = prompt.shape[1]
    table = table.T
    return pl.pallas_call(
        functools.partial(relay_kernel, n, chunks),
        out_shape=jax.ShapeDtypeStruct((rows, q_cols * n), jnp.bfloat16),
        in_specs=[hbm] * 8,
        out_specs=vmem,
        scratch_shapes=[
            pltpu.SMEM(table.shape, table.dtype),
            pltpu.SMEM(lens.shape, lens.dtype),
            pltpu.SMEM(slot.shape, slot.dtype),
            pltpu.VMEM(hidden.shape, jnp.bfloat16),
            pltpu.VMEM((rows, q_cols * n), jnp.bfloat16),
            pltpu.VMEM((rows, kv_cols * n), jnp.bfloat16),
            pltpu.VMEM((plen, kv_cols * n), jnp.bfloat16),
            pltpu.VMEM(prompt.shape, jnp.bfloat16),
            pltpu.VMEM(pool.shape, jnp.bfloat16),
            pltpu.VMEM((seqs, KEY_VALUE_HEADS * 2 * GROUP, KEY_VALUE_HEADS * HEAD_SIZE), jnp.bfloat16),
            pltpu.VMEM((KEY_VALUE_HEADS, rows * GROUP, HEAD_SIZE), jnp.bfloat16),
            pltpu.VMEM((n * rows, depth), jnp.bfloat16),
            pltpu.VMEM((depth, q_cols), jnp.bfloat16),
            pltpu.VMEM((depth, kv_cols), jnp.bfloat16),
            pltpu.VMEM((n * rows, q_cols), jnp.float32),
            pltpu.VMEM((n * rows, kv_cols), jnp.float32),
            pltpu.VMEM((n * rows, q_cols), jnp.bfloat16),
            pltpu.VMEM((n * rows, kv_cols), jnp.bfloat16),
            dma((half, chunks)),
            dma((half, chunks)),
            dma((half, chunks)),
            dma((half, chunks)),
            dma((n,)),
            dma((n,)),
            dma((n,)),
            dma((n,)),
            dma((n,)),
            dma((n,)),
            dma((2, chunks)),
            dma((6,)),
        ],
        compiler_params=pltpu.CompilerParams(
            collective_id=0, has_side_effects=True, vmem_limit_bytes=60 << 20
        ),
        name="relay",
    )(table, lens, slot, hidden, wq, wkv, prompt, pool)


def exchange(hidden, wq, wkv, prompt_kv):
    prompt = lax.all_to_all(prompt_kv, "tensor", split_axis=0, concat_axis=2, tiled=True)[0]
    gathered = lax.all_gather(hidden, "tensor", axis=0, tiled=True)
    outs = []
    for w in (wq, wkv):
        part = jnp.dot(gathered, w, preferred_element_type=jnp.float32).astype(jnp.bfloat16)
        outs.append(lax.all_to_all(part, "tensor", split_axis=0, concat_axis=1, tiled=True))
    return outs[0], outs[1], prompt


def per_device(n, hidden, wq, wkv, cache_pool, page_table, ctx_len, prompt_slot, prompt_kv):
    seqs = hidden.shape[0]
    flat = hidden.reshape(seqs * 2, hidden.shape[2])
    aligned = wq.shape[1] % 128 == 0 and wkv.shape[1] % 128 == 0
    if aligned and n % 2 == 0 and n > 4 and flat.shape[0] % 16 == 0 and prompt_kv.shape[0] == n:
        out = relay(hidden, wq, wkv, prompt_kv, cache_pool, page_table, ctx_len, prompt_slot, n)
    else:
        query, keyval, prompt = exchange(flat, wq, wkv, prompt_kv)
        out = attend(query, keyval, prompt, cache_pool, page_table, ctx_len, prompt_slot)
    return out.reshape(seqs, 2, out.shape[1])


def solution(mesh):
    placed = (
        P(("groups", "tensor", "batch"), None, None),
        P(None, "tensor"),
        P(None, "tensor"),
        P(("groups", "tensor", "batch"), None, None),
        P(("groups", "tensor", "batch"), None),
        P(("groups", "tensor", "batch")),
        P(("groups", "tensor", "batch")),
        P(("groups", "batch"), None, "tensor"),
    )
    return jax.shard_map(
        functools.partial(per_device, mesh.shape["tensor"]),
        mesh=mesh,
        in_specs=placed,
        out_specs=P(("groups", "tensor", "batch"), None, None),
        check_vma=False,
    )
```

```python
import functools

import jax
import jax.numpy as jnp
from jax import lax
from jax.experimental import pallas as pl
from jax.experimental.pallas import tpu as pltpu
from jax.sharding import PartitionSpec as P

QUERY_HEADS = 64
KEY_VALUE_HEADS = 8
HEAD_SIZE = 128
GROUP = QUERY_HEADS // KEY_VALUE_HEADS
MESH = pl.DeviceIdType.MESH
NEG = -1e30
UNROLL = 2


def dot_t(a, b):
    return lax.dot_general(a, b, (((1,), (1,)), ((), ())), preferred_element_type=jnp.float32)


def attend_kernel(
    seqs, pages, table, lens, slot, *refs
):
    page_refs = refs[:pages]
    q_ref, kv_ref, prompt_ref, out_ref, qp, op = refs[pages:]
    s = pl.program_id(0)
    rows = seqs * 2
    block = 2 * GROUP
    total = rows * GROUP
    kv_half = KEY_VALUE_HEADS * HEAD_SIZE

    def perm(transposed):
        r = lax.broadcasted_iota(jnp.int32, (total, total), 1 if transposed else 0)
        c = lax.broadcasted_iota(jnp.int32, (total, total), 0 if transposed else 1)
        seq, rest = r // block, r % block
        source = (rest % GROUP) * rows + seq * 2 + rest // GROUP
        return jnp.where(c == source, 1.0, 0.0).astype(jnp.bfloat16)

    @pl.when(s == 0)
    def _():
        p = perm(False)
        for h in range(KEY_VALUE_HEADS):
            tiles = [
                q_ref[:, (h * GROUP + g) * HEAD_SIZE : (h * GROUP + g + 1) * HEAD_SIZE]
                for g in range(GROUP)
            ]
            stacked = jnp.concatenate(tiles, axis=0)
            qp[h] = jnp.dot(p, stacked, preferred_element_type=jnp.float32).astype(jnp.bfloat16)

    page_rows = page_refs[0].shape[1]
    length = lens[s]
    lane = lax.broadcasted_iota(jnp.int32, (block, page_rows), 1)
    new_col = lax.broadcasted_iota(jnp.int32, (block, rows), 1)
    new_row = lax.broadcasted_iota(jnp.int32, (block, rows), 0)
    new_live = (new_col // 2 == s) & (new_col % 2 <= new_row // GROUP)
    here = pl.ds(pl.multiple_of(s * block, block), block)
    scale = HEAD_SIZE ** (-0.5)

    def heads(with_prompt):
        for h in range(KEY_VALUE_HEADS):
            kc = slice(h * HEAD_SIZE, (h + 1) * HEAD_SIZE)
            vc = slice(kv_half + h * HEAD_SIZE, kv_half + (h + 1) * HEAD_SIZE)
            qh = qp[h, here, :]
            parts = []
            for p in range(pages):
                sc = dot_t(qh, page_refs[p][0, :, kc]) * scale
                parts.append((jnp.where(lane + p * page_rows < length, sc, NEG), page_refs[p][0, :, vc]))
            sc = dot_t(qh, kv_ref[:, kc]) * scale
            parts.append((jnp.where(new_live, sc, NEG), kv_ref[:, vc]))
            if with_prompt:
                parts.append((dot_t(qh, prompt_ref[:, kc]) * scale, prompt_ref[:, vc]))
            top = functools.reduce(
                jnp.maximum, [jnp.max(sc, axis=-1, keepdims=True) for sc, _ in parts]
            )
            expo = [jnp.exp(sc - top) for sc, _ in parts]
            norm = functools.reduce(
                jnp.add, [jnp.sum(e, axis=-1, keepdims=True) for e in expo]
            )
            acc = functools.reduce(
                jnp.add,
                [
                    jnp.dot(e.astype(jnp.bfloat16), v, preferred_element_type=jnp.float32)
                    for e, (_, v) in zip(expo, parts)
                ],
            )
            op[h, here, :] = (acc / norm).astype(jnp.bfloat16)

    mine = s == slot[0]

    @pl.when(mine)
    def _():
        heads(True)

    @pl.when(jnp.logical_not(mine))
    def _():
        heads(False)

    @pl.when(s == seqs - 1)
    def _():
        p = perm(True)
        for h in range(KEY_VALUE_HEADS):
            back = jnp.dot(p, op[h], preferred_element_type=jnp.float32).astype(jnp.bfloat16)
            for g in range(GROUP):
                out_ref[:, (h * GROUP + g) * HEAD_SIZE : (h * GROUP + g + 1) * HEAD_SIZE] = back[
                    g * rows : (g + 1) * rows, :
                ]


def attend(query, keyval, prompt, pool, table, lens, slot):
    seqs, pages = table.shape
    page_rows, kv_cols = pool.shape[1:]
    rows = query.shape[0]

    def page_spec(p):
        return pl.BlockSpec((1, page_rows, kv_cols), lambda s, t, l, sl: (t[s * pages + p], 0, 0))

    def whole(x):
        return pl.BlockSpec(x.shape, lambda s, t, l, sl: (0,) * x.ndim)

    total = rows * GROUP
    return pl.pallas_call(
        functools.partial(attend_kernel, seqs, pages),
        grid_spec=pltpu.PrefetchScalarGridSpec(
            num_scalar_prefetch=3,
            grid=(seqs,),
            in_specs=[page_spec(p) for p in range(pages)] + [whole(query), whole(keyval), whole(prompt)],
            out_specs=pl.BlockSpec(query.shape, lambda s, t, l, sl: (0, 0)),
            scratch_shapes=[
                pltpu.VMEM((KEY_VALUE_HEADS, total, HEAD_SIZE), jnp.bfloat16),
                pltpu.VMEM((KEY_VALUE_HEADS, total, HEAD_SIZE), jnp.bfloat16),
            ],
        ),
        out_shape=jax.ShapeDtypeStruct(query.shape, jnp.bfloat16),
        compiler_params=pltpu.CompilerParams(dimension_semantics=("arbitrary",)),
        name="attend",
    )(table.reshape(-1), lens, slot, *([pool] * pages), query, keyval, prompt)


def attend_resident(table, lens, slot, pool_v, q_out, kv_out, prompt_out, qbd, op, out, after):
    seqs = lens.shape[0]
    pages = table.shape[0]
    rows = seqs * 2
    block = 2 * GROUP
    total = rows * GROUP
    kv_half = KEY_VALUE_HEADS * HEAD_SIZE
    page_rows = pool_v.shape[1]
    lanes = KEY_VALUE_HEADS * block
    scale = HEAD_SIZE ** (-0.5)

    def perm(transposed):
        r = lax.broadcasted_iota(jnp.int32, (total, total), 1 if transposed else 0)
        c = lax.broadcasted_iota(jnp.int32, (total, total), 0 if transposed else 1)
        seq, rest = r // block, r % block
        source = (rest % GROUP) * rows + seq * 2 + rest // GROUP
        return jnp.where(c == source, 1.0, 0.0).astype(jnp.bfloat16)

    p = perm(False)
    for h in range(KEY_VALUE_HEADS):
        tiles = [
            q_out[:, (h * GROUP + g) * HEAD_SIZE : (h * GROUP + g + 1) * HEAD_SIZE]
            for g in range(GROUP)
        ]
        ordered = jnp.dot(
            p, jnp.concatenate(tiles, axis=0), preferred_element_type=jnp.float32
        ).astype(jnp.bfloat16)
        for s in range(seqs):
            qbd[s, h * block : (h + 1) * block, h * HEAD_SIZE : (h + 1) * HEAD_SIZE] = ordered[
                s * block : (s + 1) * block, :
            ]

    key = lax.broadcasted_iota(jnp.int32, (page_rows, lanes), 0)
    new_key = lax.broadcasted_iota(jnp.int32, (rows, lanes), 0)
    new_pos = lax.broadcasted_iota(jnp.int32, (rows, lanes), 1) // GROUP % 2

    def one(s, with_prompt):
        q = qbd[s]
        where_pages = [table[p, s] for p in range(pages)]
        parts = []
        for p in range(pages):
            sc = dot_t(pool_v[where_pages[p], :, :kv_half], q) * scale
            parts.append(jnp.where(key + p * page_rows < lens[s], sc, NEG))
        if with_prompt:
            parts.append(dot_t(prompt_out[:, :kv_half], q) * scale)
        sc = dot_t(kv_out[:, :kv_half], q) * scale
        parts.append(jnp.where((new_key // 2 == s) & (new_key % 2 <= new_pos), sc, NEG))
        top = functools.reduce(jnp.maximum, [jnp.max(x, axis=0, keepdims=True) for x in parts])
        expo = [jnp.exp(x - top) for x in parts]
        norm = functools.reduce(jnp.add, [jnp.sum(e, axis=0, keepdims=True) for e in expo])
        weights = [jnp.transpose(e / norm).astype(jnp.bfloat16) for e in expo]
        wide = jnp.concatenate(weights[:pages], axis=1)
        outs = []
        for h in range(KEY_VALUE_HEADS):
            vc = slice(kv_half + h * HEAD_SIZE, kv_half + (h + 1) * HEAD_SIZE)
            mine = slice(h * block, (h + 1) * block)
            v = jnp.concatenate([pool_v[w, :, vc] for w in where_pages], axis=0)
            acc = jnp.dot(wide[mine], v, preferred_element_type=jnp.float32)
            acc += jnp.dot(weights[-1][mine], kv_out[:, vc], preferred_element_type=jnp.float32)
            if with_prompt:
                acc += jnp.dot(weights[pages][mine], prompt_out[:, vc], preferred_element_type=jnp.float32)
            outs.append(acc.astype(jnp.bfloat16))
        return outs

    def several(k, carry):
        for u in range(UNROLL):
            s = k * UNROLL + u
            for h, o in enumerate(one(s, False)):
                op[h, pl.ds(pl.multiple_of(s * block, block), block), :] = o
        return carry

    lax.fori_loop(0, seqs // UNROLL, several, 0)
    after()
    chosen = slot[0]
    continued = one(chosen, True)
    row_seq = lax.broadcasted_iota(jnp.int32, (total, HEAD_SIZE), 0) // block
    p = perm(True)
    for h in range(KEY_VALUE_HEADS):
        spread = jnp.concatenate([continued[h]] * seqs, axis=0)
        mixed = jnp.where(row_seq == chosen, spread, op[h])
        back = jnp.dot(p, mixed, preferred_element_type=jnp.float32).astype(jnp.bfloat16)
        for g in range(GROUP):
            out[:, (h * GROUP + g) * HEAD_SIZE : (h * GROUP + g + 1) * HEAD_SIZE] = back[
                g * rows : (g + 1) * rows, :
            ]


def relay_kernel(
    n, chunks, table_h, lens_h, slot_h, hidden, wq, wkv, prompt, pool, attended,
    table, lens, slot, hid_v,
    q_out, kv_out, prompt_out, prompt_v, pool_v, qbd, op,
    gath, wq_v, wkv_v, acc_q, acc_kv, stage_q, stage_kv,
    own_send, z_send, z_recv, y_send, y_recv,
    q_send, q_recv, kv_send, kv_recv, p_send, p_recv, w_sem, local_sem,
):
    me = lax.axis_index("tensor")
    rows, depth = attended.shape[0], hidden.shape[2]
    width = depth // chunks
    q_cols, kv_cols = wq.shape[1], wkv.shape[1]
    length = n // 2
    z, y = me // 2, me % 2
    partner = 2 * z + 1 - y
    last = length - 1

    def order(at, block):
        gap = jnp.abs(at - block)
        nearer = jnp.minimum(gap - 1, at) + jnp.minimum(gap - 1, last - at)
        tied = jnp.where((block > at) & (gap <= at), 1, 0)
        return 1 + nearer + tied

    def held(r):
        block = 0
        for b in range(length):
            block += jnp.where((order(z, b) == r) & (z != b), b, 0)
        return block

    blocks = [z] + [held(r) for r in range(1, length)]
    onward = [None] + [jnp.where(b < z, z + 1, z - 1) for b in blocks[1:]]

    def rows_of(k, count=1):
        return pl.ds(k * rows, count * rows)

    def cols_of(c):
        return pl.ds(pl.multiple_of(c * width, width), width)

    barrier = pltpu.get_barrier_semaphore()

    def greet(t):
        pl.semaphore_signal(barrier, inc=1, device_id={"tensor": t}, device_id_type=MESH)

    greet(partner)
    pl.when(z > 0)(lambda: greet(me - 2))
    pl.when(z < last)(lambda: greet(me + 2))

    own = pltpu.make_async_copy(hidden, hid_v, local_sem.at[0])
    own.start()
    scalars = []
    for k, (src, dst) in enumerate(((table_h, table), (lens_h, lens), (slot_h, slot))):
        copy = pltpu.make_async_copy(src, dst, local_sem.at[1 + k])
        copy.start()
        scalars.append(copy)

    def weight_copies(c):
        k = cols_of(c)
        return (
            pltpu.make_async_copy(wq.at[k, :], wq_v.at[k, :], w_sem.at[0, c]),
            pltpu.make_async_copy(wkv.at[k, :], wkv_v.at[k, :], w_sem.at[1, c]),
        )

    for c in range(chunks):
        for copy in weight_copies(c):
            copy.start()
    load_prompt = pltpu.make_async_copy(prompt, prompt_v, local_sem.at[4])
    load_prompt.start()
    load_pool = pltpu.make_async_copy(pool, pool_v, local_sem.at[5])
    load_pool.start()

    def z_copy(r, c, dest, slot_there, send):
        return pltpu.make_async_remote_copy(
            src_ref=gath.at[rows_of(2 * r), cols_of(c)],
            dst_ref=gath.at[rows_of(2 * slot_there), cols_of(c)],
            send_sem=send,
            recv_sem=z_recv.at[slot_there, c],
            device_id={"tensor": 2 * dest + y},
            device_id_type=MESH,
        )

    def own_copy(side, c):
        dest = z - 1 if side == 0 else z + 1
        return z_copy(0, c, dest, order(dest, z), own_send.at[side, c])

    def forward(r, c):
        dest = onward[r]
        return z_copy(r, c, dest, order(dest, blocks[r]), z_send.at[r, c])

    def z_arrival(r, c):
        return z_copy(r, c, jnp.where(z == 0, 1, z - 1), r, z_send.at[r, c])

    def y_copy(r, c):
        return pltpu.make_async_remote_copy(
            src_ref=gath.at[rows_of(2 * r), cols_of(c)],
            dst_ref=gath.at[rows_of(2 * r + 1), cols_of(c)],
            send_sem=y_send.at[r, c],
            recv_sem=y_recv.at[r, c],
            device_id={"tensor": partner},
            device_id_type=MESH,
        )

    def has_onward(r):
        return (onward[r] >= 0) & (onward[r] <= last)

    acc_q[...] = jnp.zeros_like(acc_q)
    acc_kv[...] = jnp.zeros_like(acc_kv)
    qbd[...] = jnp.zeros_like(qbd)
    own.wait()
    for c in range(chunks):
        cols = slice(c * width, (c + 1) * width)
        gath[rows_of(0), cols] = hid_v[:, :, cols].reshape(rows, width)
    pl.semaphore_wait(barrier, 1 + jnp.where(z > 0, 1, 0) + jnp.where(z < last, 1, 0))

    for c in range(chunks):
        pl.when(z > 0)(lambda c=c: own_copy(0, c).start())
        pl.when(z < last)(lambda c=c: own_copy(1, c).start())
        y_copy(0, c).start()

    def phase(r):
        first, count = (0, 3) if r == 0 else (2 * r + 1, 2 if r < last else 1)
        taken = slice(first * rows, (first + count) * rows)

        def step(c, carry):
            if r < last:
                z_arrival(r + 1, c).wait_recv()
                pl.when(has_onward(r + 1))(lambda: forward(r + 1, c).start())
                y_copy(r + 1, c).start()
            y_copy(r, c).wait_recv()
            if r == 0:
                for copy in weight_copies(c):
                    copy.wait()
            x = gath[taken, cols_of(c)]
            for w, acc in ((wq_v, acc_q), (wkv_v, acc_kv)):
                acc[taken, :] += jnp.dot(x, w[cols_of(c), :], preferred_element_type=jnp.float32)
            return carry

        lax.fori_loop(0, chunks, step, 0)
        stage_q[taken, :] = acc_q[taken, :].astype(jnp.bfloat16)
        stage_kv[taken, :] = acc_kv[taken, :].astype(jnp.bfloat16)

    sends = []

    def hand_out(k):
        t = 2 * blocks[k // 2] + (y if k % 2 == 0 else 1 - y)
        for stage, out, cols, send, recv in (
            (stage_q, q_out, q_cols, q_send, q_recv),
            (stage_kv, kv_out, kv_cols, kv_send, kv_recv),
        ):
            copy = pltpu.make_async_remote_copy(
                src_ref=stage.at[rows_of(k), :],
                dst_ref=out.at[:, pl.ds(pl.multiple_of(me * cols, cols), cols)],
                send_sem=send.at[k],
                recv_sem=recv.at[me],
                device_id={"tensor": t},
                device_id_type=MESH,
            )
            copy.start()
            sends.append(copy)

    def prompt_copy(k):
        t = 2 * blocks[k // 2] + (y if k % 2 == 0 else 1 - y)
        return pltpu.make_async_remote_copy(
            src_ref=prompt_v.at[t],
            dst_ref=prompt_out.at[:, pl.ds(pl.multiple_of(me * kv_cols, kv_cols), kv_cols)],
            send_sem=p_send.at[k],
            recv_sem=p_recv.at[me],
            device_id={"tensor": t},
            device_id_type=MESH,
        )

    for r in range(length):
        phase(r)
        if r < last:
            hand_out(2 * r + 2)
        if r == last - 1:
            load_prompt.wait()
            for k in range(1, n - 1, 2):
                hand_out(k)
            for k in range(2, n, 2):
                copy = prompt_copy(k)
                copy.start()
                sends.append(copy)
    hand_out(n - 1)
    for k in range(1, n, 2):
        copy = prompt_copy(k)
        copy.start()
        sends.append(copy)

    for source, out, cols in (
        (stage_q[0:rows, :], q_out, q_cols),
        (stage_kv[0:rows, :], kv_out, kv_cols),
        (prompt_v[me], prompt_out, kv_cols),
    ):
        out[:, pl.ds(pl.multiple_of(me * cols, cols), cols)] = source

    def arrival(out, cols, recv, d):
        t = lax.rem(me + d, n)
        here = out.at[:, pl.ds(pl.multiple_of(t * cols, cols), cols)]
        return pltpu.make_async_remote_copy(
            src_ref=here, dst_ref=here, send_sem=recv.at[t], recv_sem=recv.at[t],
            device_id={"tensor": t}, device_id_type=MESH,
        )

    for d in range(1, n):
        arrival(q_out, q_cols, q_recv, d).wait_recv()
        arrival(kv_out, kv_cols, kv_recv, d).wait_recv()
    for copy in scalars:
        copy.wait()
    load_pool.wait()

    def after():
        for d in range(1, n):
            arrival(prompt_out, kv_cols, p_recv, d).wait_recv()

    attend_resident(
        table, lens, slot, pool_v, q_out, kv_out, prompt_out, qbd, op, attended, after
    )
    for copy in sends:
        copy.wait_send()

    def drain(c, carry):
        pl.when(z > 0)(lambda: own_copy(0, c).wait_send())
        pl.when(z < last)(lambda: own_copy(1, c).wait_send())
        for r in range(length):
            y_copy(r, c).wait_send()
            if r > 0:
                pl.when(has_onward(r))(lambda r=r: forward(r, c).wait_send())
        return carry

    lax.fori_loop(0, chunks, drain, 0)


def relay(hidden, wq, wkv, prompt, pool, table, lens, slot, n):
    seqs, per, depth = hidden.shape
    rows = seqs * per
    q_cols, kv_cols = wq.shape[1], wkv.shape[1]
    chunks = 8
    half = n // 2
    vmem = pl.BlockSpec(memory_space=pltpu.VMEM)
    hbm = pl.BlockSpec(memory_space=pltpu.HBM)
    dma = pltpu.SemaphoreType.DMA
    plen = prompt.shape[1]
    table = table.T
    return pl.pallas_call(
        functools.partial(relay_kernel, n, chunks),
        out_shape=jax.ShapeDtypeStruct((rows, q_cols * n), jnp.bfloat16),
        in_specs=[hbm] * 8,
        out_specs=vmem,
        scratch_shapes=[
            pltpu.SMEM(table.shape, table.dtype),
            pltpu.SMEM(lens.shape, lens.dtype),
            pltpu.SMEM(slot.shape, slot.dtype),
            pltpu.VMEM(hidden.shape, jnp.bfloat16),
            pltpu.VMEM((rows, q_cols * n), jnp.bfloat16),
            pltpu.VMEM((rows, kv_cols * n), jnp.bfloat16),
            pltpu.VMEM((plen, kv_cols * n), jnp.bfloat16),
            pltpu.VMEM(prompt.shape, jnp.bfloat16),
            pltpu.VMEM(pool.shape, jnp.bfloat16),
            pltpu.VMEM((seqs, KEY_VALUE_HEADS * 2 * GROUP, KEY_VALUE_HEADS * HEAD_SIZE), jnp.bfloat16),
            pltpu.VMEM((KEY_VALUE_HEADS, rows * GROUP, HEAD_SIZE), jnp.bfloat16),
            pltpu.VMEM((n * rows, depth), jnp.bfloat16),
            pltpu.VMEM((depth, q_cols), jnp.bfloat16),
            pltpu.VMEM((depth, kv_cols), jnp.bfloat16),
            pltpu.VMEM((n * rows, q_cols), jnp.float32),
            pltpu.VMEM((n * rows, kv_cols), jnp.float32),
            pltpu.VMEM((n * rows, q_cols), jnp.bfloat16),
            pltpu.VMEM((n * rows, kv_cols), jnp.bfloat16),
            dma((2, chunks)),
            dma((half, chunks)),
            dma((half, chunks)),
            dma((half, chunks)),
            dma((half, chunks)),
            dma((n,)),
            dma((n,)),
            dma((n,)),
            dma((n,)),
            dma((n,)),
            dma((n,)),
            dma((2, chunks)),
            dma((6,)),
        ],
        compiler_params=pltpu.CompilerParams(
            collective_id=0, has_side_effects=True, vmem_limit_bytes=60 << 20
        ),
        name="relay",
    )(table, lens, slot, hidden, wq, wkv, prompt, pool)


def exchange(hidden, wq, wkv, prompt_kv):
    prompt = lax.all_to_all(prompt_kv, "tensor", split_axis=0, concat_axis=2, tiled=True)[0]
    gathered = lax.all_gather(hidden, "tensor", axis=0, tiled=True)
    outs = []
    for w in (wq, wkv):
        part = jnp.dot(gathered, w, preferred_element_type=jnp.float32).astype(jnp.bfloat16)
        outs.append(lax.all_to_all(part, "tensor", split_axis=0, concat_axis=1, tiled=True))
    return outs[0], outs[1], prompt


def per_device(n, hidden, wq, wkv, cache_pool, page_table, ctx_len, prompt_slot, prompt_kv):
    seqs = hidden.shape[0]
    flat = hidden.reshape(seqs * 2, hidden.shape[2])
    aligned = wq.shape[1] % 128 == 0 and wkv.shape[1] % 128 == 0
    if aligned and n % 2 == 0 and n > 4 and flat.shape[0] % 16 == 0 and prompt_kv.shape[0] == n:
        out = relay(hidden, wq, wkv, prompt_kv, cache_pool, page_table, ctx_len, prompt_slot, n)
    else:
        query, keyval, prompt = exchange(flat, wq, wkv, prompt_kv)
        out = attend(query, keyval, prompt, cache_pool, page_table, ctx_len, prompt_slot)
    return out.reshape(seqs, 2, out.shape[1])


def solution(mesh):
    placed = (
        P(("groups", "tensor", "batch"), None, None),
        P(None, "tensor"),
        P(None, "tensor"),
        P(("groups", "tensor", "batch"), None, None),
        P(("groups", "tensor", "batch"), None),
        P(("groups", "tensor", "batch")),
        P(("groups", "tensor", "batch")),
        P(("groups", "batch"), None, "tensor"),
    )
    return jax.shard_map(
        functools.partial(per_device, mesh.shape["tensor"]),
        mesh=mesh,
        in_specs=placed,
        out_specs=P(("groups", "tensor", "batch"), None, None),
        check_vma=False,
    )
```

```python
import functools

import jax
import jax.numpy as jnp
from jax import lax
from jax.experimental import pallas as pl
from jax.experimental.pallas import tpu as pltpu
from jax.sharding import PartitionSpec as P

QUERY_HEADS = 64
KEY_VALUE_HEADS = 8
HEAD_SIZE = 128
GROUP = QUERY_HEADS // KEY_VALUE_HEADS
MESH = pl.DeviceIdType.MESH
NEG = -1e30
UNROLL = 2


def dot_t(a, b):
    return lax.dot_general(a, b, (((1,), (1,)), ((), ())), preferred_element_type=jnp.float32)


def attend_kernel(
    seqs, pages, table, lens, slot, *refs
):
    page_refs = refs[:pages]
    q_ref, kv_ref, prompt_ref, out_ref, qp, op = refs[pages:]
    s = pl.program_id(0)
    rows = seqs * 2
    block = 2 * GROUP
    total = rows * GROUP
    kv_half = KEY_VALUE_HEADS * HEAD_SIZE

    def perm(transposed):
        r = lax.broadcasted_iota(jnp.int32, (total, total), 1 if transposed else 0)
        c = lax.broadcasted_iota(jnp.int32, (total, total), 0 if transposed else 1)
        seq, rest = r // block, r % block
        source = (rest % GROUP) * rows + seq * 2 + rest // GROUP
        return jnp.where(c == source, 1.0, 0.0).astype(jnp.bfloat16)

    @pl.when(s == 0)
    def _():
        p = perm(False)
        for h in range(KEY_VALUE_HEADS):
            tiles = [
                q_ref[:, (h * GROUP + g) * HEAD_SIZE : (h * GROUP + g + 1) * HEAD_SIZE]
                for g in range(GROUP)
            ]
            stacked = jnp.concatenate(tiles, axis=0)
            qp[h] = jnp.dot(p, stacked, preferred_element_type=jnp.float32).astype(jnp.bfloat16)

    page_rows = page_refs[0].shape[1]
    length = lens[s]
    lane = lax.broadcasted_iota(jnp.int32, (block, page_rows), 1)
    new_col = lax.broadcasted_iota(jnp.int32, (block, rows), 1)
    new_row = lax.broadcasted_iota(jnp.int32, (block, rows), 0)
    new_live = (new_col // 2 == s) & (new_col % 2 <= new_row // GROUP)
    here = pl.ds(pl.multiple_of(s * block, block), block)
    scale = HEAD_SIZE ** (-0.5)

    def heads(with_prompt):
        for h in range(KEY_VALUE_HEADS):
            kc = slice(h * HEAD_SIZE, (h + 1) * HEAD_SIZE)
            vc = slice(kv_half + h * HEAD_SIZE, kv_half + (h + 1) * HEAD_SIZE)
            qh = qp[h, here, :]
            parts = []
            for p in range(pages):
                sc = dot_t(qh, page_refs[p][0, :, kc]) * scale
                parts.append((jnp.where(lane + p * page_rows < length, sc, NEG), page_refs[p][0, :, vc]))
            sc = dot_t(qh, kv_ref[:, kc]) * scale
            parts.append((jnp.where(new_live, sc, NEG), kv_ref[:, vc]))
            if with_prompt:
                parts.append((dot_t(qh, prompt_ref[:, kc]) * scale, prompt_ref[:, vc]))
            top = functools.reduce(
                jnp.maximum, [jnp.max(sc, axis=-1, keepdims=True) for sc, _ in parts]
            )
            expo = [jnp.exp(sc - top) for sc, _ in parts]
            norm = functools.reduce(
                jnp.add, [jnp.sum(e, axis=-1, keepdims=True) for e in expo]
            )
            acc = functools.reduce(
                jnp.add,
                [
                    jnp.dot(e.astype(jnp.bfloat16), v, preferred_element_type=jnp.float32)
                    for e, (_, v) in zip(expo, parts)
                ],
            )
            op[h, here, :] = (acc / norm).astype(jnp.bfloat16)

    mine = s == slot[0]

    @pl.when(mine)
    def _():
        heads(True)

    @pl.when(jnp.logical_not(mine))
    def _():
        heads(False)

    @pl.when(s == seqs - 1)
    def _():
        p = perm(True)
        for h in range(KEY_VALUE_HEADS):
            back = jnp.dot(p, op[h], preferred_element_type=jnp.float32).astype(jnp.bfloat16)
            for g in range(GROUP):
                out_ref[:, (h * GROUP + g) * HEAD_SIZE : (h * GROUP + g + 1) * HEAD_SIZE] = back[
                    g * rows : (g + 1) * rows, :
                ]


def attend(query, keyval, prompt, pool, table, lens, slot):
    seqs, pages = table.shape
    page_rows, kv_cols = pool.shape[1:]
    rows = query.shape[0]

    def page_spec(p):
        return pl.BlockSpec((1, page_rows, kv_cols), lambda s, t, l, sl: (t[s * pages + p], 0, 0))

    def whole(x):
        return pl.BlockSpec(x.shape, lambda s, t, l, sl: (0,) * x.ndim)

    total = rows * GROUP
    return pl.pallas_call(
        functools.partial(attend_kernel, seqs, pages),
        grid_spec=pltpu.PrefetchScalarGridSpec(
            num_scalar_prefetch=3,
            grid=(seqs,),
            in_specs=[page_spec(p) for p in range(pages)] + [whole(query), whole(keyval), whole(prompt)],
            out_specs=pl.BlockSpec(query.shape, lambda s, t, l, sl: (0, 0)),
            scratch_shapes=[
                pltpu.VMEM((KEY_VALUE_HEADS, total, HEAD_SIZE), jnp.bfloat16),
                pltpu.VMEM((KEY_VALUE_HEADS, total, HEAD_SIZE), jnp.bfloat16),
            ],
        ),
        out_shape=jax.ShapeDtypeStruct(query.shape, jnp.bfloat16),
        compiler_params=pltpu.CompilerParams(dimension_semantics=("arbitrary",)),
        name="attend",
    )(table.reshape(-1), lens, slot, *([pool] * pages), query, keyval, prompt)


def attend_resident(table, lens, slot, pool_v, q_out, kv_out, prompt_out, qbd, op, out, after):
    seqs = lens.shape[0]
    pages = table.shape[0]
    rows = seqs * 2
    block = 2 * GROUP
    total = rows * GROUP
    kv_half = KEY_VALUE_HEADS * HEAD_SIZE
    page_rows = pool_v.shape[1]
    lanes = KEY_VALUE_HEADS * block
    scale = HEAD_SIZE ** (-0.5)

    def perm(transposed):
        r = lax.broadcasted_iota(jnp.int32, (total, total), 1 if transposed else 0)
        c = lax.broadcasted_iota(jnp.int32, (total, total), 0 if transposed else 1)
        seq, rest = r // block, r % block
        source = (rest % GROUP) * rows + seq * 2 + rest // GROUP
        return jnp.where(c == source, 1.0, 0.0).astype(jnp.bfloat16)

    p = perm(False)
    for h in range(KEY_VALUE_HEADS):
        tiles = [
            q_out[:, (h * GROUP + g) * HEAD_SIZE : (h * GROUP + g + 1) * HEAD_SIZE]
            for g in range(GROUP)
        ]
        ordered = jnp.dot(
            p, jnp.concatenate(tiles, axis=0), preferred_element_type=jnp.float32
        ).astype(jnp.bfloat16)
        for s in range(seqs):
            qbd[s, h * block : (h + 1) * block, h * HEAD_SIZE : (h + 1) * HEAD_SIZE] = ordered[
                s * block : (s + 1) * block, :
            ]

    key = lax.broadcasted_iota(jnp.int32, (page_rows, lanes), 0)
    new_key = lax.broadcasted_iota(jnp.int32, (rows, lanes), 0)
    new_pos = lax.broadcasted_iota(jnp.int32, (rows, lanes), 1) // GROUP % 2

    def one(s, with_prompt):
        q = qbd[s]
        where_pages = [table[p, s] for p in range(pages)]
        parts = []
        for p in range(pages):
            sc = dot_t(pool_v[where_pages[p], :, :kv_half], q) * scale
            parts.append(jnp.where(key + p * page_rows < lens[s], sc, NEG))
        if with_prompt:
            parts.append(dot_t(prompt_out[:, :kv_half], q) * scale)
        sc = dot_t(kv_out[:, :kv_half], q) * scale
        parts.append(jnp.where((new_key // 2 == s) & (new_key % 2 <= new_pos), sc, NEG))
        top = functools.reduce(jnp.maximum, [jnp.max(x, axis=0, keepdims=True) for x in parts])
        expo = [jnp.exp(x - top) for x in parts]
        norm = functools.reduce(jnp.add, [jnp.sum(e, axis=0, keepdims=True) for e in expo])
        weights = [jnp.transpose(e / norm).astype(jnp.bfloat16) for e in expo]
        wide = jnp.concatenate(weights[:pages], axis=1)
        outs = []
        for h in range(KEY_VALUE_HEADS):
            vc = slice(kv_half + h * HEAD_SIZE, kv_half + (h + 1) * HEAD_SIZE)
            mine = slice(h * block, (h + 1) * block)
            v = jnp.concatenate([pool_v[w, :, vc] for w in where_pages], axis=0)
            acc = jnp.dot(wide[mine], v, preferred_element_type=jnp.float32)
            acc += jnp.dot(weights[-1][mine], kv_out[:, vc], preferred_element_type=jnp.float32)
            if with_prompt:
                acc += jnp.dot(weights[pages][mine], prompt_out[:, vc], preferred_element_type=jnp.float32)
            outs.append(acc.astype(jnp.bfloat16))
        return outs

    def several(k, carry):
        for u in range(UNROLL):
            s = k * UNROLL + u
            for h, o in enumerate(one(s, False)):
                op[h, pl.ds(pl.multiple_of(s * block, block), block), :] = o
        return carry

    lax.fori_loop(0, seqs // UNROLL, several, 0)
    after()
    chosen = slot[0]
    continued = one(chosen, True)
    row_seq = lax.broadcasted_iota(jnp.int32, (total, HEAD_SIZE), 0) // block
    p = perm(True)
    for h in range(KEY_VALUE_HEADS):
        spread = jnp.concatenate([continued[h]] * seqs, axis=0)
        mixed = jnp.where(row_seq == chosen, spread, op[h])
        back = jnp.dot(p, mixed, preferred_element_type=jnp.float32).astype(jnp.bfloat16)
        for g in range(GROUP):
            out[:, (h * GROUP + g) * HEAD_SIZE : (h * GROUP + g + 1) * HEAD_SIZE] = back[
                g * rows : (g + 1) * rows, :
            ]


def relay_kernel(
    n, chunks, table_h, lens_h, slot_h, hidden, wq, wkv, prompt, pool, attended,
    table, lens, slot, hid_v,
    q_out, kv_out, prompt_out, prompt_v, pool_v, qbd, op,
    gath, wq_v, wkv_v, acc_q, acc_kv, stage_q, stage_kv,
    own_send, z_send, z_recv, y_send, y_recv,
    q_send, q_recv, kv_send, kv_recv, p_send, p_recv, w_sem, local_sem,
):
    me = lax.axis_index("tensor")
    rows, depth = attended.shape[0], hidden.shape[2]
    width = depth // chunks
    q_cols, kv_cols = wq.shape[1], wkv.shape[1]
    length = n // 2
    z, y = me // 2, me % 2
    partner = 2 * z + 1 - y
    last = length - 1

    def order(at, block):
        gap = jnp.abs(at - block)
        nearer = jnp.minimum(gap - 1, at) + jnp.minimum(gap - 1, last - at)
        both = (gap <= at) & (gap <= last - at)
        favoured = (block > at) == (at % 2 == 0)
        return 1 + nearer + jnp.where(both & jnp.logical_not(favoured), 1, 0)

    def held(r):
        block = 0
        for b in range(length):
            block += jnp.where((order(z, b) == r) & (z != b), b, 0)
        return block

    groups = [[(0, 0), (1, 0), (0, 1), (0, 2)]]
    groups[0] += [(1, 1)]
    groups += [[(1, r), (0, r + 1)] for r in range(2, last)]
    groups += [[(1, last)]]
    seats = [seat for group in groups for seat in group]
    place = {seat: k for k, seat in enumerate(seats)}
    z_place = [place[0, r] for r in range(length)]
    y_place = [place[1, r] for r in range(length)]

    def place_there(slot_there):
        found = 0
        for r in range(1, length):
            found += jnp.where(slot_there == r, z_place[r], 0)
        return found

    blocks = [z] + [held(r) for r in range(1, length)]
    onward = [None] + [jnp.where(b < z, z + 1, z - 1) for b in blocks[1:]]

    def rows_of(k, count=1):
        return pl.ds(k * rows, count * rows)

    def cols_of(c):
        return pl.ds(pl.multiple_of(c * width, width), width)

    barrier = pltpu.get_barrier_semaphore()

    def greet(t):
        pl.semaphore_signal(barrier, inc=1, device_id={"tensor": t}, device_id_type=MESH)

    greet(partner)
    pl.when(z > 0)(lambda: greet(me - 2))
    pl.when(z < last)(lambda: greet(me + 2))

    own = pltpu.make_async_copy(hidden, hid_v, local_sem.at[0])
    own.start()
    scalars = []
    for k, (src, dst) in enumerate(((table_h, table), (lens_h, lens), (slot_h, slot))):
        copy = pltpu.make_async_copy(src, dst, local_sem.at[1 + k])
        copy.start()
        scalars.append(copy)

    weights = (
        pltpu.make_async_copy(wq, wq_v, w_sem.at[0]),
        pltpu.make_async_copy(wkv, wkv_v, w_sem.at[1]),
    )
    for copy in weights:
        copy.start()
    load_prompt = pltpu.make_async_copy(prompt, prompt_v, local_sem.at[4])
    load_pool = pltpu.make_async_copy(pool, pool_v, local_sem.at[5])

    def z_copy(r, c, dest, slot_there, send):
        return pltpu.make_async_remote_copy(
            src_ref=gath.at[rows_of(z_place[r]), cols_of(c)],
            dst_ref=gath.at[rows_of(place_there(slot_there)), cols_of(c)],
            send_sem=send,
            recv_sem=z_recv.at[slot_there, c],
            device_id={"tensor": 2 * dest + y},
            device_id_type=MESH,
        )

    def own_copy(side, c):
        dest = z - 1 if side == 0 else z + 1
        return z_copy(0, c, dest, order(dest, z), own_send.at[side, c])

    def forward(r, c):
        dest = onward[r]
        return z_copy(r, c, dest, order(dest, blocks[r]), z_send.at[r, c])

    def z_arrival(r, c):
        return z_copy(r, c, jnp.where(z == 0, 1, z - 1), r, z_send.at[r, c])

    def y_copy(r, c):
        return pltpu.make_async_remote_copy(
            src_ref=gath.at[rows_of(z_place[r]), cols_of(c)],
            dst_ref=gath.at[rows_of(y_place[r]), cols_of(c)],
            send_sem=y_send.at[r, c],
            recv_sem=y_recv.at[r, c],
            device_id={"tensor": partner},
            device_id_type=MESH,
        )

    def has_onward(r):
        return (onward[r] >= 0) & (onward[r] <= last)

    acc_q[...] = jnp.zeros_like(acc_q)
    acc_kv[...] = jnp.zeros_like(acc_kv)
    qbd[...] = jnp.zeros_like(qbd)
    own.wait()
    for c in range(chunks):
        cols = slice(c * width, (c + 1) * width)
        gath[rows_of(0), cols] = hid_v[:, :, cols].reshape(rows, width)
    pl.semaphore_wait(barrier, 1 + jnp.where(z > 0, 1, 0) + jnp.where(z < last, 1, 0))

    for c in range(chunks):
        pl.when(z > 0)(lambda c=c: own_copy(0, c).start())
        pl.when(z < last)(lambda c=c: own_copy(1, c).start())
        y_copy(0, c).start()

    def phase(r):
        if r == 1:
            for copy in weights:
                copy.wait()
            load_prompt.start()
            load_pool.start()
        group = groups[max(r - 1, 0)]
        first = place[group[0]]
        taken = slice(first * rows, (first + len(group)) * rows)

        def step(c, carry):
            if r < last:
                z_arrival(r + 1, c).wait_recv()
                pl.when(has_onward(r + 1))(lambda: forward(r + 1, c).start())
                y_copy(r + 1, c).start()
            y_copy(r, c).wait_recv()
            if r == 0:
                return carry
            x = gath[taken, cols_of(c)]
            for w, acc in ((wq_v, acc_q), (wkv_v, acc_kv)):
                acc[taken, :] += jnp.dot(x, w[cols_of(c), :], preferred_element_type=jnp.float32)
            return carry

        lax.fori_loop(0, chunks, step, 0)
        if r > 0:
            stage_q[taken, :] = acc_q[taken, :].astype(jnp.bfloat16)
            stage_kv[taken, :] = acc_kv[taken, :].astype(jnp.bfloat16)

    sends = []

    def owner(seat):
        return 2 * blocks[seat[1]] + (y if seat[0] == 0 else 1 - y)

    def hand_out(seat):
        k, t = place[seat], owner(seat)
        for stage, out, cols, send, recv in (
            (stage_q, q_out, q_cols, q_send, q_recv),
            (stage_kv, kv_out, kv_cols, kv_send, kv_recv),
        ):
            copy = pltpu.make_async_remote_copy(
                src_ref=stage.at[rows_of(k), :],
                dst_ref=out.at[:, pl.ds(pl.multiple_of(me * cols, cols), cols)],
                send_sem=send.at[k],
                recv_sem=recv.at[me],
                device_id={"tensor": t},
                device_id_type=MESH,
            )
            copy.start()
            sends.append(copy)

    def send_prompt(seat):
        k, t = place[seat], owner(seat)
        copy = pltpu.make_async_remote_copy(
            src_ref=prompt_v.at[t],
            dst_ref=prompt_out.at[:, pl.ds(pl.multiple_of(me * kv_cols, kv_cols), kv_cols)],
            send_sem=p_send.at[k],
            recv_sem=p_recv.at[me],
            device_id={"tensor": t},
            device_id_type=MESH,
        )
        copy.start()
        sends.append(copy)

    for r in range(length):
        phase(r)
        if r < last:
            for seat in groups[r - 1] if r > 0 else []:
                if seat[0] == 0 and seat[1] > 0:
                    hand_out(seat)
        if r == last - 1:
            load_prompt.wait()
            for q in range(0, last):
                hand_out((1, q))
            for q in range(1, length):
                send_prompt((0, q))
    hand_out((1, last))
    for q in range(length):
        send_prompt((1, q))

    for source, out, cols in (
        (stage_q[0:rows, :], q_out, q_cols),
        (stage_kv[0:rows, :], kv_out, kv_cols),
        (prompt_v[me], prompt_out, kv_cols),
    ):
        out[:, pl.ds(pl.multiple_of(me * cols, cols), cols)] = source

    def arrival(out, cols, recv, d):
        t = lax.rem(me + d, n)
        here = out.at[:, pl.ds(pl.multiple_of(t * cols, cols), cols)]
        return pltpu.make_async_remote_copy(
            src_ref=here, dst_ref=here, send_sem=recv.at[t], recv_sem=recv.at[t],
            device_id={"tensor": t}, device_id_type=MESH,
        )

    for d in range(1, n):
        arrival(q_out, q_cols, q_recv, d).wait_recv()
        arrival(kv_out, kv_cols, kv_recv, d).wait_recv()
    for copy in scalars:
        copy.wait()
    load_pool.wait()

    def after():
        for d in range(1, n):
            arrival(prompt_out, kv_cols, p_recv, d).wait_recv()

    attend_resident(
        table, lens, slot, pool_v, q_out, kv_out, prompt_out, qbd, op, attended, after
    )
    for copy in sends:
        copy.wait_send()

    def drain(c, carry):
        pl.when(z > 0)(lambda: own_copy(0, c).wait_send())
        pl.when(z < last)(lambda: own_copy(1, c).wait_send())
        for r in range(length):
            y_copy(r, c).wait_send()
            if r > 0:
                pl.when(has_onward(r))(lambda r=r: forward(r, c).wait_send())
        return carry

    lax.fori_loop(0, chunks, drain, 0)


def relay(hidden, wq, wkv, prompt, pool, table, lens, slot, n):
    seqs, per, depth = hidden.shape
    rows = seqs * per
    q_cols, kv_cols = wq.shape[1], wkv.shape[1]
    chunks = 8
    half = n // 2
    vmem = pl.BlockSpec(memory_space=pltpu.VMEM)
    hbm = pl.BlockSpec(memory_space=pltpu.HBM)
    dma = pltpu.SemaphoreType.DMA
    plen = prompt.shape[1]
    table = table.T
    return pl.pallas_call(
        functools.partial(relay_kernel, n, chunks),
        out_shape=jax.ShapeDtypeStruct((rows, q_cols * n), jnp.bfloat16),
        in_specs=[hbm] * 8,
        out_specs=vmem,
        scratch_shapes=[
            pltpu.SMEM(table.shape, table.dtype),
            pltpu.SMEM(lens.shape, lens.dtype),
            pltpu.SMEM(slot.shape, slot.dtype),
            pltpu.VMEM(hidden.shape, jnp.bfloat16),
            pltpu.VMEM((rows, q_cols * n), jnp.bfloat16),
            pltpu.VMEM((rows, kv_cols * n), jnp.bfloat16),
            pltpu.VMEM((plen, kv_cols * n), jnp.bfloat16),
            pltpu.VMEM(prompt.shape, jnp.bfloat16),
            pltpu.VMEM(pool.shape, jnp.bfloat16),
            pltpu.VMEM((seqs, KEY_VALUE_HEADS * 2 * GROUP, KEY_VALUE_HEADS * HEAD_SIZE), jnp.bfloat16),
            pltpu.VMEM((KEY_VALUE_HEADS, rows * GROUP, HEAD_SIZE), jnp.bfloat16),
            pltpu.VMEM((n * rows, depth), jnp.bfloat16),
            pltpu.VMEM((depth, q_cols), jnp.bfloat16),
            pltpu.VMEM((depth, kv_cols), jnp.bfloat16),
            pltpu.VMEM((n * rows, q_cols), jnp.float32),
            pltpu.VMEM((n * rows, kv_cols), jnp.float32),
            pltpu.VMEM((n * rows, q_cols), jnp.bfloat16),
            pltpu.VMEM((n * rows, kv_cols), jnp.bfloat16),
            dma((2, chunks)),
            dma((half, chunks)),
            dma((half, chunks)),
            dma((half, chunks)),
            dma((half, chunks)),
            dma((n,)),
            dma((n,)),
            dma((n,)),
            dma((n,)),
            dma((n,)),
            dma((n,)),
            dma((2,)),
            dma((6,)),
        ],
        compiler_params=pltpu.CompilerParams(
            collective_id=0, has_side_effects=True, vmem_limit_bytes=60 << 20
        ),
        name="relay",
    )(table, lens, slot, hidden, wq, wkv, prompt, pool)


def exchange(hidden, wq, wkv, prompt_kv):
    prompt = lax.all_to_all(prompt_kv, "tensor", split_axis=0, concat_axis=2, tiled=True)[0]
    gathered = lax.all_gather(hidden, "tensor", axis=0, tiled=True)
    outs = []
    for w in (wq, wkv):
        part = jnp.dot(gathered, w, preferred_element_type=jnp.float32).astype(jnp.bfloat16)
        outs.append(lax.all_to_all(part, "tensor", split_axis=0, concat_axis=1, tiled=True))
    return outs[0], outs[1], prompt


def per_device(n, hidden, wq, wkv, cache_pool, page_table, ctx_len, prompt_slot, prompt_kv):
    seqs = hidden.shape[0]
    flat = hidden.reshape(seqs * 2, hidden.shape[2])
    aligned = wq.shape[1] % 128 == 0 and wkv.shape[1] % 128 == 0
    if aligned and n % 4 == 0 and n > 4 and flat.shape[0] % 16 == 0 and prompt_kv.shape[0] == n:
        out = relay(hidden, wq, wkv, prompt_kv, cache_pool, page_table, ctx_len, prompt_slot, n)
    else:
        query, keyval, prompt = exchange(flat, wq, wkv, prompt_kv)
        out = attend(query, keyval, prompt, cache_pool, page_table, ctx_len, prompt_slot)
    return out.reshape(seqs, 2, out.shape[1])


def solution(mesh):
    placed = (
        P(("groups", "tensor", "batch"), None, None),
        P(None, "tensor"),
        P(None, "tensor"),
        P(("groups", "tensor", "batch"), None, None),
        P(("groups", "tensor", "batch"), None),
        P(("groups", "tensor", "batch")),
        P(("groups", "tensor", "batch")),
        P(("groups", "batch"), None, "tensor"),
    )
    return jax.shard_map(
        functools.partial(per_device, mesh.shape["tensor"]),
        mesh=mesh,
        in_specs=placed,
        out_specs=P(("groups", "tensor", "batch"), None, None),
        check_vma=False,
    )
```

```python
import functools

import jax
import jax.numpy as jnp
from jax import lax
from jax.experimental import pallas as pl
from jax.experimental.pallas import tpu as pltpu
from jax.sharding import PartitionSpec as P

QUERY_HEADS = 64
KEY_VALUE_HEADS = 8
HEAD_SIZE = 128
GROUP = QUERY_HEADS // KEY_VALUE_HEADS
MESH = pl.DeviceIdType.MESH
NEG = -1e30


def dot_t(a, b):
    return lax.dot_general(a, b, (((1,), (1,)), ((), ())), preferred_element_type=jnp.float32)


def attend_kernel(
    seqs, pages, table, lens, slot, *refs
):
    page_refs = refs[:pages]
    q_ref, kv_ref, prompt_ref, out_ref, qp, op = refs[pages:]
    s = pl.program_id(0)
    rows = seqs * 2
    block = 2 * GROUP
    total = rows * GROUP
    kv_half = KEY_VALUE_HEADS * HEAD_SIZE

    def perm(transposed):
        r = lax.broadcasted_iota(jnp.int32, (total, total), 1 if transposed else 0)
        c = lax.broadcasted_iota(jnp.int32, (total, total), 0 if transposed else 1)
        seq, rest = r // block, r % block
        source = (rest % GROUP) * rows + seq * 2 + rest // GROUP
        return jnp.where(c == source, 1.0, 0.0).astype(jnp.bfloat16)

    @pl.when(s == 0)
    def _():
        p = perm(False)
        for h in range(KEY_VALUE_HEADS):
            tiles = [
                q_ref[:, (h * GROUP + g) * HEAD_SIZE : (h * GROUP + g + 1) * HEAD_SIZE]
                for g in range(GROUP)
            ]
            stacked = jnp.concatenate(tiles, axis=0)
            qp[h] = jnp.dot(p, stacked, preferred_element_type=jnp.float32).astype(jnp.bfloat16)

    page_rows = page_refs[0].shape[1]
    length = lens[s]
    lane = lax.broadcasted_iota(jnp.int32, (block, page_rows), 1)
    new_col = lax.broadcasted_iota(jnp.int32, (block, rows), 1)
    new_row = lax.broadcasted_iota(jnp.int32, (block, rows), 0)
    new_live = (new_col // 2 == s) & (new_col % 2 <= new_row // GROUP)
    here = pl.ds(pl.multiple_of(s * block, block), block)
    scale = HEAD_SIZE ** (-0.5)

    def heads(with_prompt):
        for h in range(KEY_VALUE_HEADS):
            kc = slice(h * HEAD_SIZE, (h + 1) * HEAD_SIZE)
            vc = slice(kv_half + h * HEAD_SIZE, kv_half + (h + 1) * HEAD_SIZE)
            qh = qp[h, here, :]
            parts = []
            for p in range(pages):
                sc = dot_t(qh, page_refs[p][0, :, kc]) * scale
                parts.append((jnp.where(lane + p * page_rows < length, sc, NEG), page_refs[p][0, :, vc]))
            sc = dot_t(qh, kv_ref[:, kc]) * scale
            parts.append((jnp.where(new_live, sc, NEG), kv_ref[:, vc]))
            if with_prompt:
                parts.append((dot_t(qh, prompt_ref[:, kc]) * scale, prompt_ref[:, vc]))
            top = functools.reduce(
                jnp.maximum, [jnp.max(sc, axis=-1, keepdims=True) for sc, _ in parts]
            )
            expo = [jnp.exp(sc - top) for sc, _ in parts]
            norm = functools.reduce(
                jnp.add, [jnp.sum(e, axis=-1, keepdims=True) for e in expo]
            )
            acc = functools.reduce(
                jnp.add,
                [
                    jnp.dot(e.astype(jnp.bfloat16), v, preferred_element_type=jnp.float32)
                    for e, (_, v) in zip(expo, parts)
                ],
            )
            op[h, here, :] = (acc / norm).astype(jnp.bfloat16)

    mine = s == slot[0]

    @pl.when(mine)
    def _():
        heads(True)

    @pl.when(jnp.logical_not(mine))
    def _():
        heads(False)

    @pl.when(s == seqs - 1)
    def _():
        p = perm(True)
        for h in range(KEY_VALUE_HEADS):
            back = jnp.dot(p, op[h], preferred_element_type=jnp.float32).astype(jnp.bfloat16)
            for g in range(GROUP):
                out_ref[:, (h * GROUP + g) * HEAD_SIZE : (h * GROUP + g + 1) * HEAD_SIZE] = back[
                    g * rows : (g + 1) * rows, :
                ]


def attend(query, keyval, prompt, pool, table, lens, slot):
    seqs, pages = table.shape
    page_rows, kv_cols = pool.shape[1:]
    rows = query.shape[0]

    def page_spec(p):
        return pl.BlockSpec((1, page_rows, kv_cols), lambda s, t, l, sl: (t[s * pages + p], 0, 0))

    def whole(x):
        return pl.BlockSpec(x.shape, lambda s, t, l, sl: (0,) * x.ndim)

    total = rows * GROUP
    return pl.pallas_call(
        functools.partial(attend_kernel, seqs, pages),
        grid_spec=pltpu.PrefetchScalarGridSpec(
            num_scalar_prefetch=3,
            grid=(seqs,),
            in_specs=[page_spec(p) for p in range(pages)] + [whole(query), whole(keyval), whole(prompt)],
            out_specs=pl.BlockSpec(query.shape, lambda s, t, l, sl: (0, 0)),
            scratch_shapes=[
                pltpu.VMEM((KEY_VALUE_HEADS, total, HEAD_SIZE), jnp.bfloat16),
                pltpu.VMEM((KEY_VALUE_HEADS, total, HEAD_SIZE), jnp.bfloat16),
            ],
        ),
        out_shape=jax.ShapeDtypeStruct(query.shape, jnp.bfloat16),
        compiler_params=pltpu.CompilerParams(dimension_semantics=("arbitrary",)),
        name="attend",
    )(table.reshape(-1), lens, slot, *([pool] * pages), query, keyval, prompt)


def attend_resident(
    table, lens, slot, pool_v, q_out, kv_out, prompt_out, qbd, ubd, qh, held, stat, op, out,
    parity, first_half, second_half, after,
):
    seqs = lens.shape[0]
    pages = table.shape[0]
    rows = seqs * 2
    block = 2 * GROUP
    total = rows * GROUP
    kv_half = KEY_VALUE_HEADS * HEAD_SIZE
    page_rows = pool_v.shape[1]
    lanes = KEY_VALUE_HEADS * block
    scale = HEAD_SIZE ** (-0.5)

    def perm(transposed):
        r = lax.broadcasted_iota(jnp.int32, (total, total), 1 if transposed else 0)
        c = lax.broadcasted_iota(jnp.int32, (total, total), 0 if transposed else 1)
        seq, rest = r // block, r % block
        source = (rest % GROUP) * rows + seq * 2 + rest // GROUP
        return jnp.where(c == source, 1.0, 0.0).astype(jnp.bfloat16)

    pairs = seqs // 2
    side = KEY_VALUE_HEADS // 2

    def head(e, par):
        return 2 * (e % side) + par

    def head_cols(e, par, base=0):
        return pl.ds(pl.multiple_of(base + head(e, par) * HEAD_SIZE, HEAD_SIZE), HEAD_SIZE)

    def spread_queries(half, par):
        p = perm(False)
        for e in range(side):
            h = head(e, par)
            tiles = [
                q_out[:, pl.ds(pl.multiple_of((h * GROUP + g) * HEAD_SIZE, HEAD_SIZE), HEAD_SIZE)]
                for g in range(GROUP)
            ]
            ordered = jnp.dot(
                p, jnp.concatenate(tiles, axis=0), preferred_element_type=jnp.float32
            ).astype(jnp.bfloat16)
            qh[h] = ordered
            for s in range(seqs):
                piece = ordered[s * block : (s + 1) * block, :]
                qbd[s, pl.ds(pl.multiple_of(h * block, block), block), head_cols(e, par)] = piece
                k = s % 2 * side + e
                ubd[
                    half * pairs + s // 2,
                    k * block : (k + 1) * block,
                    k * HEAD_SIZE : (k + 1) * HEAD_SIZE,
                ] = piece

    key = lax.broadcasted_iota(jnp.int32, (page_rows, lanes), 0)
    new_key = lax.broadcasted_iota(jnp.int32, (rows, lanes), 0)
    new_pos = lax.broadcasted_iota(jnp.int32, (rows, lanes), 1) // GROUP % 2

    def one(s, with_prompt):
        q = qbd[s]
        where_pages = [table[p, s] for p in range(pages)]
        parts = []
        for p in range(pages):
            sc = dot_t(pool_v[where_pages[p], :, :kv_half], q) * scale
            parts.append(jnp.where(key + p * page_rows < lens[s], sc, NEG))
        if with_prompt:
            parts.append(dot_t(prompt_out[:, :kv_half], q) * scale)
        sc = dot_t(kv_out[:, :kv_half], q) * scale
        parts.append(jnp.where((new_key // 2 == s) & (new_key % 2 <= new_pos), sc, NEG))
        top = functools.reduce(jnp.maximum, [jnp.max(x, axis=0, keepdims=True) for x in parts])
        expo = [jnp.exp(x - top) for x in parts]
        norm = functools.reduce(jnp.add, [jnp.sum(e, axis=0, keepdims=True) for e in expo])
        weights = [jnp.transpose(e / norm).astype(jnp.bfloat16) for e in expo]
        wide = jnp.concatenate(weights[:pages], axis=1)
        outs = []
        for h in range(KEY_VALUE_HEADS):
            vc = slice(kv_half + h * HEAD_SIZE, kv_half + (h + 1) * HEAD_SIZE)
            mine = slice(h * block, (h + 1) * block)
            v = jnp.concatenate([pool_v[w, :, vc] for w in where_pages], axis=0)
            acc = jnp.dot(wide[mine], v, preferred_element_type=jnp.float32)
            acc += jnp.dot(weights[-1][mine], kv_out[:, vc], preferred_element_type=jnp.float32)
            if with_prompt:
                acc += jnp.dot(weights[pages][mine], prompt_out[:, vc], preferred_element_type=jnp.float32)
            outs.append(acc.astype(jnp.bfloat16))
        return outs

    lane_seq = lax.broadcasted_iota(jnp.int32, (1, lanes), 1) // (side * block)

    def cache_part(half, k, par):
        q = ubd[half * pairs + k]
        spots = [[table[p, 2 * k + u] for u in range(2)] for p in range(pages)]
        limit = jnp.where(lane_seq == 0, lens[2 * k], lens[2 * k + 1])
        parts = []
        for p in range(pages):
            keys = [pool_v[spots[p][e // side], :, head_cols(e, par)] for e in range(2 * side)]
            sc = dot_t(jnp.concatenate(keys, axis=1), q) * scale
            parts.append(jnp.where(key + p * page_rows < limit, sc, NEG))
        top = functools.reduce(jnp.maximum, [jnp.max(x, axis=0, keepdims=True) for x in parts])
        expo = [jnp.exp(x - top) for x in parts]
        norm = functools.reduce(jnp.add, [jnp.sum(e, axis=0, keepdims=True) for e in expo])
        wide = jnp.concatenate([jnp.transpose(e).astype(jnp.bfloat16) for e in expo], axis=1)
        tops = jnp.transpose(jnp.broadcast_to(top, (8, lanes)))
        norms = jnp.transpose(jnp.broadcast_to(norm, (8, lanes)))
        for e in range(2 * side):
            v = jnp.concatenate(
                [pool_v[spots[p][e // side], :, head_cols(e, par, kv_half)] for p in range(pages)],
                axis=0,
            )
            mine = slice(e * block, (e + 1) * block)
            there = pl.ds(pl.multiple_of((2 * k + e // side) * block, block), block)
            stat[head(e, par), there, 0:8] = tops[mine]
            stat[head(e, par), there, 8:16] = norms[mine]
            held[head(e, par), there, :] = jnp.dot(wide[mine], v, preferred_element_type=jnp.float32)

    def merge():
        row = lax.broadcasted_iota(jnp.int32, (total, rows), 0)
        col = lax.broadcasted_iota(jnp.int32, (total, rows), 1)
        live = (col // 2 == row // block) & (col % 2 <= row // GROUP % 2)
        heads = range(KEY_VALUE_HEADS)
        scores = [
            dot_t(qh[h], kv_out[:, h * HEAD_SIZE : (h + 1) * HEAD_SIZE]) * scale for h in heads
        ]
        scores = [jnp.where(live, sc, NEG) for sc in scores]
        tops = [
            jnp.maximum(stat[h, :, 0:1], jnp.max(scores[h], axis=1, keepdims=True)) for h in heads
        ]
        shrinks = [jnp.exp(stat[h, :, 0:1] - tops[h]) for h in heads]
        expos = [jnp.exp(scores[h] - tops[h]) for h in heads]
        norms = [
            shrinks[h] * stat[h, :, 8:9] + jnp.sum(expos[h], axis=1, keepdims=True) for h in heads
        ]
        fresh = [
            jnp.dot(
                (expos[h] / norms[h]).astype(jnp.bfloat16),
                kv_out[:, kv_half + h * HEAD_SIZE : kv_half + (h + 1) * HEAD_SIZE],
                preferred_element_type=jnp.float32,
            )
            for h in heads
        ]
        for h in heads:
            op[h] = (held[h] * (shrinks[h] / norms[h]) + fresh[h]).astype(jnp.bfloat16)

    def sweep(part, half, par):
        def step(k, carry):
            part(half, k, par)
            return carry

        lax.fori_loop(0, pairs, step, 0, unroll=4)

    first_half()
    spread_queries(0, parity)
    sweep(cache_part, 0, parity)
    second_half()
    spread_queries(1, 1 - parity)
    sweep(cache_part, 1, 1 - parity)
    merge()
    after()
    chosen = slot[0]
    continued = one(chosen, True)
    row_seq = lax.broadcasted_iota(jnp.int32, (total, HEAD_SIZE), 0) // block
    p = perm(True)
    for h in range(KEY_VALUE_HEADS):
        spread = jnp.concatenate([continued[h]] * seqs, axis=0)
        mixed = jnp.where(row_seq == chosen, spread, op[h])
        back = jnp.dot(p, mixed, preferred_element_type=jnp.float32).astype(jnp.bfloat16)
        for g in range(GROUP):
            out[:, (h * GROUP + g) * HEAD_SIZE : (h * GROUP + g + 1) * HEAD_SIZE] = back[
                g * rows : (g + 1) * rows, :
            ]


def relay_kernel(
    n, chunks, table_h, lens_h, slot_h, hidden, wq, wkv, prompt, pool, attended,
    table, lens, slot, hid_v,
    q_out, kv_out, prompt_out, prompt_v, pool_v, qbd, ubd, qh, held_acc, stat, op,
    gath, wq_v, wkv_v, acc_q, acc_kv, stage_q, stage_kv,
    own_send, z_send, z_recv, y_send, y_recv,
    q_send, q_recv, kv_send, kv_recv, p_send, p_recv, w_sem, local_sem,
):
    me = lax.axis_index("tensor")
    rows, depth = attended.shape[0], hidden.shape[2]
    width = depth // chunks
    q_cols, kv_cols = wq.shape[1], wkv.shape[1]
    length = n // 2
    z, y = me // 2, me % 2
    partner = 2 * z + 1 - y
    last = length - 1

    def order(at, block):
        gap = jnp.abs(at - block)
        nearer = jnp.minimum(gap - 1, at) + jnp.minimum(gap - 1, last - at)
        both = (gap <= at) & (gap <= last - at)
        favoured = (block > at) == (at % 2 == 0)
        return 1 + nearer + jnp.where(both & jnp.logical_not(favoured), 1, 0)

    def held(r):
        block = 0
        for b in range(length):
            block += jnp.where((order(z, b) == r) & (z != b), b, 0)
        return block

    groups = [[(0, 0), (1, 0), (0, 1), (0, 2)]]
    groups[0] += [(1, 1)]
    groups += [[(1, r), (0, r + 1)] for r in range(2, last)]
    groups += [[(1, last)]]
    seats = [seat for group in groups for seat in group]
    place = {seat: k for k, seat in enumerate(seats)}
    z_place = [place[0, r] for r in range(length)]
    y_place = [place[1, r] for r in range(length)]

    def place_there(slot_there):
        found = 0
        for r in range(1, length):
            found += jnp.where(slot_there == r, z_place[r], 0)
        return found

    blocks = [z] + [held(r) for r in range(1, length)]
    onward = [None] + [jnp.where(b < z, z + 1, z - 1) for b in blocks[1:]]

    def rows_of(k, count=1):
        return pl.ds(k * rows, count * rows)

    def cols_of(c):
        return pl.ds(pl.multiple_of(c * width, width), width)

    barrier = pltpu.get_barrier_semaphore()

    def greet(t):
        pl.semaphore_signal(barrier, inc=1, device_id={"tensor": t}, device_id_type=MESH)

    greet(partner)
    pl.when(z > 0)(lambda: greet(me - 2))
    pl.when(z < last)(lambda: greet(me + 2))

    own = pltpu.make_async_copy(hidden, hid_v, local_sem.at[0])
    own.start()
    scalars = []
    for k, (src, dst) in enumerate(((table_h, table), (lens_h, lens), (slot_h, slot))):
        copy = pltpu.make_async_copy(src, dst, local_sem.at[1 + k])
        copy.start()
        scalars.append(copy)

    weights = (
        pltpu.make_async_copy(wq, wq_v, w_sem.at[0]),
        pltpu.make_async_copy(wkv, wkv_v, w_sem.at[1]),
    )
    for copy in weights:
        copy.start()
    load_prompt = pltpu.make_async_copy(prompt, prompt_v, local_sem.at[4])
    load_pool = pltpu.make_async_copy(pool, pool_v, local_sem.at[5])

    def z_copy(r, c, dest, slot_there, send):
        return pltpu.make_async_remote_copy(
            src_ref=gath.at[rows_of(z_place[r]), cols_of(c)],
            dst_ref=gath.at[rows_of(place_there(slot_there)), cols_of(c)],
            send_sem=send,
            recv_sem=z_recv.at[slot_there, c],
            device_id={"tensor": 2 * dest + y},
            device_id_type=MESH,
        )

    def own_copy(side, c):
        dest = z - 1 if side == 0 else z + 1
        return z_copy(0, c, dest, order(dest, z), own_send.at[side, c])

    def forward(r, c):
        dest = onward[r]
        return z_copy(r, c, dest, order(dest, blocks[r]), z_send.at[r, c])

    def z_arrival(r, c):
        return z_copy(r, c, jnp.where(z == 0, 1, z - 1), r, z_send.at[r, c])

    def y_copy(r, c):
        return pltpu.make_async_remote_copy(
            src_ref=gath.at[rows_of(z_place[r]), cols_of(c)],
            dst_ref=gath.at[rows_of(y_place[r]), cols_of(c)],
            send_sem=y_send.at[r, c],
            recv_sem=y_recv.at[r, c],
            device_id={"tensor": partner},
            device_id_type=MESH,
        )

    def has_onward(r):
        return (onward[r] >= 0) & (onward[r] <= last)

    acc_q[...] = jnp.zeros_like(acc_q)
    acc_kv[...] = jnp.zeros_like(acc_kv)
    qbd[...] = jnp.zeros_like(qbd)
    ubd[...] = jnp.zeros_like(ubd)
    own.wait()
    for c in range(chunks):
        cols = slice(c * width, (c + 1) * width)
        gath[rows_of(0), cols] = hid_v[:, :, cols].reshape(rows, width)
    pl.semaphore_wait(barrier, 1 + jnp.where(z > 0, 1, 0) + jnp.where(z < last, 1, 0))

    for c in range(chunks):
        pl.when(z > 0)(lambda c=c: own_copy(0, c).start())
        pl.when(z < last)(lambda c=c: own_copy(1, c).start())
        y_copy(0, c).start()

    def phase(r):
        if r == 1:
            for copy in weights:
                copy.wait()
            load_prompt.start()
            load_pool.start()
        group = groups[max(r - 1, 0)]
        first = place[group[0]]
        taken = slice(first * rows, (first + len(group)) * rows)

        def step(c, carry):
            if r < last:
                z_arrival(r + 1, c).wait_recv()
                pl.when(has_onward(r + 1))(lambda: forward(r + 1, c).start())
                y_copy(r + 1, c).start()
            y_copy(r, c).wait_recv()
            if r == 0:
                return carry
            x = gath[taken, cols_of(c)]
            for w, acc in ((wq_v, acc_q), (wkv_v, acc_kv)):
                acc[taken, :] += jnp.dot(x, w[cols_of(c), :], preferred_element_type=jnp.float32)
            return carry

        lax.fori_loop(0, chunks, step, 0)
        if r > 0:
            stage_q[taken, :] = acc_q[taken, :].astype(jnp.bfloat16)
            stage_kv[taken, :] = acc_kv[taken, :].astype(jnp.bfloat16)

    sends = []

    def owner(seat):
        return 2 * blocks[seat[1]] + (y if seat[0] == 0 else 1 - y)

    def hand_out(seat):
        k, t = place[seat], owner(seat)
        for stage, out, cols, send, recv in (
            (stage_q, q_out, q_cols, q_send, q_recv),
            (stage_kv, kv_out, kv_cols, kv_send, kv_recv),
        ):
            copy = pltpu.make_async_remote_copy(
                src_ref=stage.at[rows_of(k), :],
                dst_ref=out.at[:, pl.ds(pl.multiple_of(me * cols, cols), cols)],
                send_sem=send.at[k],
                recv_sem=recv.at[me],
                device_id={"tensor": t},
                device_id_type=MESH,
            )
            copy.start()
            sends.append(copy)

    def send_prompt(seat):
        k, t = place[seat], owner(seat)
        copy = pltpu.make_async_remote_copy(
            src_ref=prompt_v.at[t],
            dst_ref=prompt_out.at[:, pl.ds(pl.multiple_of(me * kv_cols, kv_cols), kv_cols)],
            send_sem=p_send.at[k],
            recv_sem=p_recv.at[me],
            device_id={"tensor": t},
            device_id_type=MESH,
        )
        copy.start()
        sends.append(copy)

    for r in range(length):
        phase(r)
        if r < last:
            for seat in groups[r - 1] if r > 0 else []:
                if seat[0] == 0 and seat[1] > 0:
                    hand_out(seat)
        if r == last - 1:
            load_prompt.wait()
            for q in range(0, last):
                hand_out((1, q))
            for q in range(1, length):
                send_prompt((0, q))
    hand_out((1, last))
    for q in range(length):
        send_prompt((1, q))

    for source, out, cols in (
        (stage_q[0:rows, :], q_out, q_cols),
        (stage_kv[0:rows, :], kv_out, kv_cols),
        (prompt_v[me], prompt_out, kv_cols),
    ):
        out[:, pl.ds(pl.multiple_of(me * cols, cols), cols)] = source

    def arrival(out, cols, recv, d):
        t = lax.rem(me + d, n)
        here = out.at[:, pl.ds(pl.multiple_of(t * cols, cols), cols)]
        return pltpu.make_async_remote_copy(
            src_ref=here, dst_ref=here, send_sem=recv.at[t], recv_sem=recv.at[t],
            device_id={"tensor": t}, device_id_type=MESH,
        )

    for copy in scalars:
        copy.wait()
    load_pool.wait()

    def first_half():
        for d in range(2, n, 2):
            arrival(q_out, q_cols, q_recv, d).wait_recv()

    def second_half():
        for d in range(1, n):
            if d % 2 == 1:
                arrival(q_out, q_cols, q_recv, d).wait_recv()
            arrival(kv_out, kv_cols, kv_recv, d).wait_recv()

    def after():
        for d in range(1, n):
            arrival(prompt_out, kv_cols, p_recv, d).wait_recv()

    attend_resident(
        table, lens, slot, pool_v, q_out, kv_out, prompt_out, qbd, ubd, qh, held_acc, stat, op,
        attended, y, first_half, second_half, after,
    )
    for copy in sends:
        copy.wait_send()

    def drain(c, carry):
        pl.when(z > 0)(lambda: own_copy(0, c).wait_send())
        pl.when(z < last)(lambda: own_copy(1, c).wait_send())
        for r in range(length):
            y_copy(r, c).wait_send()
            if r > 0:
                pl.when(has_onward(r))(lambda r=r: forward(r, c).wait_send())
        return carry

    lax.fori_loop(0, chunks, drain, 0)


def relay(hidden, wq, wkv, prompt, pool, table, lens, slot, n):
    seqs, per, depth = hidden.shape
    rows = seqs * per
    q_cols, kv_cols = wq.shape[1], wkv.shape[1]
    chunks = 8
    half = n // 2
    vmem = pl.BlockSpec(memory_space=pltpu.VMEM)
    hbm = pl.BlockSpec(memory_space=pltpu.HBM)
    dma = pltpu.SemaphoreType.DMA
    plen = prompt.shape[1]
    table = table.T
    return pl.pallas_call(
        functools.partial(relay_kernel, n, chunks),
        out_shape=jax.ShapeDtypeStruct((rows, q_cols * n), jnp.bfloat16),
        in_specs=[hbm] * 8,
        out_specs=vmem,
        scratch_shapes=[
            pltpu.SMEM(table.shape, table.dtype),
            pltpu.SMEM(lens.shape, lens.dtype),
            pltpu.SMEM(slot.shape, slot.dtype),
            pltpu.VMEM(hidden.shape, jnp.bfloat16),
            pltpu.VMEM((rows, q_cols * n), jnp.bfloat16),
            pltpu.VMEM((rows, kv_cols * n), jnp.bfloat16),
            pltpu.VMEM((plen, kv_cols * n), jnp.bfloat16),
            pltpu.VMEM(prompt.shape, jnp.bfloat16),
            pltpu.VMEM(pool.shape, jnp.bfloat16),
            pltpu.VMEM((seqs, KEY_VALUE_HEADS * 2 * GROUP, KEY_VALUE_HEADS * HEAD_SIZE), jnp.bfloat16),
            pltpu.VMEM((seqs, KEY_VALUE_HEADS * 2 * GROUP, KEY_VALUE_HEADS * HEAD_SIZE), jnp.bfloat16),
            pltpu.VMEM((KEY_VALUE_HEADS, rows * GROUP, HEAD_SIZE), jnp.bfloat16),
            pltpu.VMEM((KEY_VALUE_HEADS, rows * GROUP, HEAD_SIZE), jnp.float32),
            pltpu.VMEM((KEY_VALUE_HEADS, rows * GROUP, 16), jnp.float32),
            pltpu.VMEM((KEY_VALUE_HEADS, rows * GROUP, HEAD_SIZE), jnp.bfloat16),
            pltpu.VMEM((n * rows, depth), jnp.bfloat16),
            pltpu.VMEM((depth, q_cols), jnp.bfloat16),
            pltpu.VMEM((depth, kv_cols), jnp.bfloat16),
            pltpu.VMEM((n * rows, q_cols), jnp.float32),
            pltpu.VMEM((n * rows, kv_cols), jnp.float32),
            pltpu.VMEM((n * rows, q_cols), jnp.bfloat16),
            pltpu.VMEM((n * rows, kv_cols), jnp.bfloat16),
            dma((2, chunks)),
            dma((half, chunks)),
            dma((half, chunks)),
            dma((half, chunks)),
            dma((half, chunks)),
            dma((n,)),
            dma((n,)),
            dma((n,)),
            dma((n,)),
            dma((n,)),
            dma((n,)),
            dma((2,)),
            dma((6,)),
        ],
        compiler_params=pltpu.CompilerParams(
            collective_id=0, has_side_effects=True, vmem_limit_bytes=60 << 20
        ),
        name="relay",
    )(table, lens, slot, hidden, wq, wkv, prompt, pool)


def exchange(hidden, wq, wkv, prompt_kv):
    prompt = lax.all_to_all(prompt_kv, "tensor", split_axis=0, concat_axis=2, tiled=True)[0]
    gathered = lax.all_gather(hidden, "tensor", axis=0, tiled=True)
    outs = []
    for w in (wq, wkv):
        part = jnp.dot(gathered, w, preferred_element_type=jnp.float32).astype(jnp.bfloat16)
        outs.append(lax.all_to_all(part, "tensor", split_axis=0, concat_axis=1, tiled=True))
    return outs[0], outs[1], prompt


def per_device(n, hidden, wq, wkv, cache_pool, page_table, ctx_len, prompt_slot, prompt_kv):
    seqs = hidden.shape[0]
    flat = hidden.reshape(seqs * 2, hidden.shape[2])
    aligned = wq.shape[1] % 128 == 0 and wkv.shape[1] % 128 == 0
    if aligned and n == KEY_VALUE_HEADS and flat.shape[0] % 16 == 0 and prompt_kv.shape[0] == n:
        out = relay(hidden, wq, wkv, prompt_kv, cache_pool, page_table, ctx_len, prompt_slot, n)
    else:
        query, keyval, prompt = exchange(flat, wq, wkv, prompt_kv)
        out = attend(query, keyval, prompt, cache_pool, page_table, ctx_len, prompt_slot)
    return out.reshape(seqs, 2, out.shape[1])


def solution(mesh):
    placed = (
        P(("groups", "tensor", "batch"), None, None),
        P(None, "tensor"),
        P(None, "tensor"),
        P(("groups", "tensor", "batch"), None, None),
        P(("groups", "tensor", "batch"), None),
        P(("groups", "tensor", "batch")),
        P(("groups", "tensor", "batch")),
        P(("groups", "batch"), None, "tensor"),
    )
    return jax.shard_map(
        functools.partial(per_device, mesh.shape["tensor"]),
        mesh=mesh,
        in_specs=placed,
        out_specs=P(("groups", "tensor", "batch"), None, None),
        check_vma=False,
    )
```
